512 devices in a mesh: rep: 2 (over y), seq: 16 (over z), head: 8 (over x), sub: 2 (over core).
Axes of the slice: x: 8, y: 2, z: 16, core: 2. Of those that a mesh axis runs over, the one named last changes fastest.
The devices are a block of a 8x8x16 slice.
Arguments:
- tokens: bfloat16 [32, 4096], P(('rep', 'sub'), 'seq'), parts along dimension 0, may hold values from -260 to 260
- attn_gain: float32 [4096], P('seq'), may hold values from 0.1 to 1.9
- w_query: bfloat16 [4096, 4096], P('seq', 'head'), may hold values from -0.09375 to 0.09375
- key_projection_weight: bfloat16 [4096, 1024], P('seq', 'head'), may hold values from -0.375 to 0.375
- value_projection_weight: bfloat16 [4096, 1024], P('seq', 'head'), may hold values from -0.375 to 0.375
- w_attn_out: bfloat16 [4096, 4096], P('head', 'seq'), may hold values from -0.09375 to 0.09375
- cache_keys: bfloat16 [32, 8, 8192, 128], P(('rep', 'sub'), 'head', 'seq'), parts along dimension 0, may hold values from -2500 to 2500
- stored_value_cache: bfloat16 [32, 8, 8192, 128], P(('rep', 'sub'), 'head', 'seq'), parts along dimension 0, may hold values from -12 to 12
- lengths: int32 [32], P(('rep', 'sub')), parts along dimension 0, may hold values from 4096 to 8192
- positions: int32 [32], P(('rep', 'sub')), parts along dimension 0, may hold values from 0 to 8191
- mamba_gain: float32 [4096], replicated, may hold values from 0.1 to 1.9
- w_in: bfloat16 [2, 4096, 8192], P(None, None, ('seq', 'head')), may hold values from -0.09375 to 0.09375
- conv_weight: float32 [4, 8192], P(None, ('seq', 'head')), may hold values from -3 to 3
- conv_bias: float32 [8192], P(('seq', 'head')), may hold values from -0.5 to 0.5
- conv_state: float32 [32, 3, 8192], P(('rep', 'sub'), None, ('seq', 'head')), parts along dimension 0, may hold values from -6 to 6
- w_xproj: bfloat16 [8192, 288], P(('seq', 'head')), may hold values from -0.0625 to 0.0625
- w_dt: bfloat16 [256, 8192], P(None, ('seq', 'head')), may hold values from -0.375 to 0.375
- dt_bias: float32 [8192], P(('seq', 'head')), may hold values from -4 to 0
- a_log: float32 [16, 8192], P(None, ('seq', 'head')), may hold values from 0 to 2.77
- skip_gain: float32 [8192], P(('seq', 'head')), may hold values from 0.25 to 2
- ssm_state: float32 [32, 16, 8192], P(('rep', 'sub'), None, ('seq', 'head')), parts along dimension 0, may hold values from -6 to 6
- w_mamba_out: bfloat16 [8192, 4096], P(('seq', 'head')), may hold values from -0.25 to 0.25
Outputs:
- hidden_out: bfloat16 [32, 4096], P(('rep', 'sub'), 'seq'), parts along dimension 0
- new_state: float32 [32, 16, 8192], P(('rep', 'sub'), None, ('seq', 'head')), parts along dimension 0
The draws below stay inside these ranges and needn't reach their ends.
There are 2 independent parts, one for each index of `rep`. The reference program is written for one: setup_inputs(seed, part) draws one part's arguments, and reference() takes and returns one part's arrays. A program takes and returns all parts, laid end to end along the dimension named above; an argument that names none is the same for every part. Nothing has to cross between parts.
Inputs may be any that keep to these rules, and one draw needn't show every extreme that they name: Cache positions p < lengths[b] hold sequence b's past keys and values; later positions are not attended.
All inputs are finite; a program needn't handle non-finite values.
Results may differ from the reference program's by a relative error of at most 0.015.
Values may be sent and summed in bfloat16 or wider, within the bound.
A program may use at most 64 MiB of HBM per device.

```python
import math
import jax
import jax.numpy as jnp
from jax import lax

MODEL_DIMENSION = 4096
QUERY_HEADS = 32
KEY_VALUE_HEADS = 8
HEAD_SIZE = 128
DI = 8192
NSTATE = 16
DT_RANK = 256
KCONV = 4
BATCH_SEQUENCES = 16
CACHE_POSITIONS = 8192


def draw_tokens(key, part):
    base_key_rows = jax.random.fold_in(jax.random.fold_in(key, 11), 0)
    base_draw = jnp.clip(jax.random.normal(base_key_rows, (BATCH_SEQUENCES, MODEL_DIMENSION), jnp.float32), -6.0, 6.0)
    across = jnp.arange(MODEL_DIMENSION, dtype=jnp.float32) / MODEL_DIMENSION
    value_vectors = base_draw * jnp.sqrt(1.0 + 2.0 * across)[None, :]
    return value_vectors.astype(jnp.bfloat16)


def draw_cache_keys(key, part):
    base_key_rows = jax.random.fold_in(jax.random.fold_in(key, 23), 0)
    value_vectors = 2.5 * jnp.clip(jax.random.normal(base_key_rows, (BATCH_SEQUENCES, KEY_VALUE_HEADS, CACHE_POSITIONS, HEAD_SIZE), jnp.float32), -6.0, 6.0)
    return value_vectors.astype(jnp.bfloat16)


def draw_stored_value_cache(key, part):
    noise_key, common_key = jax.random.split(jax.random.fold_in(key, 37), 2)
    shape = (BATCH_SEQUENCES, KEY_VALUE_HEADS, CACHE_POSITIONS, HEAD_SIZE)
    common = jnp.clip(jax.random.normal(common_key, (BATCH_SEQUENCES, KEY_VALUE_HEADS, 1, HEAD_SIZE), jnp.float32), -4.0, 4.0)
    along = (jnp.arange(CACHE_POSITIONS, dtype=jnp.float32) / CACHE_POSITIONS)[None, None, :, None]
    noise = jnp.clip(jax.random.normal(noise_key, shape, jnp.float32), -6.0, 6.0)
    ramp = 0.3 + 0.7 * along
    return (noise + ramp * common).astype(jnp.bfloat16)


def set_ends(result, own_key, least, largest):
    dims = result.shape
    spot = [jax.random.randint(jax.random.fold_in(own_key, axis), (), 0, dims[axis]) for axis in range(len(dims))]
    result = result.at[tuple(spot)].set(least)
    longest = dims.index(max(dims))
    spot[longest] = (spot[longest] + 1) % dims[longest]
    return result.at[tuple(spot)].set(largest)


def raised(result, stream_key, source, target, shards_of, factor):
    owner, partner = [(jnp.arange(result.shape[dim]) // (result.shape[dim] // shards_of)).reshape([-1 if axis == dim else 1 for axis in range(result.ndim)]) for dim in (source, target)]
    chosen = jax.random.permutation(stream_key, shards_of)[partner]
    strong = (owner == chosen) | (owner == (partner + shards_of // 2) % shards_of)
    return jnp.where(strong, factor * result, result)


def shard_levels(stream_key, dims, shards, least, largest):
    level = 1.0
    for dim, blocks in shards:
        heights = jax.random.uniform(jax.random.fold_in(jax.random.fold_in(stream_key, 6), dim), (blocks,), jnp.float32, least / len(shards), largest / len(shards))
        level = level * jnp.repeat(jnp.exp(heights), dims[dim] // blocks).reshape((-1,) + (1,) * (len(dims) - 1 - dim))
    return level


def normal_values(own_key, extent, deviation, reach, pieces=(), held_as=jnp.bfloat16):
    array = deviation * jax.random.normal(own_key, extent, jnp.float32)
    if pieces:
        array = array * shard_levels(own_key, extent, pieces, -0.22, 0.18)
    return jnp.clip(array, -reach, reach).astype(held_as)


def bell_draw_with(own_key, shape, spread, most, pieces, heavy, kind=jnp.bfloat16):
    drawn = spread * jax.random.normal(own_key, shape, jnp.float32)
    if pieces:
        drawn = drawn * shard_levels(own_key, shape, pieces, -0.22, 0.18)
    return jnp.clip(raised(drawn, jax.random.fold_in(own_key, 3), *heavy), -most, most).astype(kind)


def setup_inputs(seed: int = 0, part: int = 0) -> dict:
    keys = jax.random.split(jax.random.key(seed), 23)
    own_keys = jax.random.split(jax.random.fold_in(keys[22], part), 23)
    tokens = draw_tokens(jax.random.fold_in(jax.random.fold_in(keys[22], part), 71), part)
    attn_gain = jnp.clip(1.0 + 0.18 * jax.random.normal(keys[1], (MODEL_DIMENSION,), jnp.float32), 0.1, 1.9)
    w_query = normal_values(keys[2], (MODEL_DIMENSION, QUERY_HEADS * HEAD_SIZE), MODEL_DIMENSION ** -0.5, 0.09375, ((0, 16), (1, 8)))
    key_projection_weight = normal_values(keys[3], (MODEL_DIMENSION, KEY_VALUE_HEADS * HEAD_SIZE), (MODEL_DIMENSION // 16) ** -0.5, 0.375, ((0, 16), (1, 8)))
    value_projection_weight = normal_values(keys[4], (MODEL_DIMENSION, KEY_VALUE_HEADS * HEAD_SIZE), (MODEL_DIMENSION // 16) ** -0.5, 0.375, ((0, 16), (1, 8)))
    w_attn_out = normal_values(keys[5], (QUERY_HEADS * HEAD_SIZE, MODEL_DIMENSION), (QUERY_HEADS * HEAD_SIZE) ** -0.5, 0.09375, ((0, 8), (1, 16)))
    cache_keys = draw_cache_keys(jax.random.fold_in(jax.random.fold_in(keys[22], part), 71), part)
    stored_value_cache = draw_stored_value_cache(jax.random.fold_in(jax.random.fold_in(keys[22], part), 71), part)
    lengths = set_ends(jax.random.randint(own_keys[8], (BATCH_SEQUENCES,), CACHE_POSITIONS // 2, CACHE_POSITIONS + 1), jax.random.fold_in(own_keys[8], 1), CACHE_POSITIONS // 2, CACHE_POSITIONS).astype(jnp.int32)
    positions = set_ends(jax.random.randint(own_keys[9], (BATCH_SEQUENCES,), 0, CACHE_POSITIONS), jax.random.fold_in(own_keys[9], 1), 0, CACHE_POSITIONS - 1).astype(jnp.int32)
    mamba_gain = jnp.clip(1.0 + 0.18 * jax.random.normal(keys[10], (MODEL_DIMENSION,), jnp.float32), 0.1, 1.9)
    w_in = normal_values(keys[11], (2, MODEL_DIMENSION, DI), MODEL_DIMENSION ** -0.5, 0.09375, ((2, 128),))
    conv_weight = normal_values(keys[12], (KCONV, DI), KCONV ** -0.5, 3.0, ((1, 128),), jnp.float32)
    conv_bias = jnp.clip(jax.random.uniform(keys[13], (DI,), jnp.float32, -0.5, 0.5) * shard_levels(keys[13], (DI,), ((0, 128),), -0.4, 0.0), -0.5, 0.5)
    conv_state = normal_values(own_keys[14], (BATCH_SEQUENCES, KCONV - 1, DI), 1.0, 6.0, ((0, 2), (2, 128)), jnp.float32)
    w_xproj = normal_values(keys[15], (DI, DT_RANK + 2 * NSTATE), DI ** -0.5, 0.0625, ((0, 128),))
    w_dt = normal_values(keys[16], (DT_RANK, DI), DT_RANK ** -0.5, 0.375, ((1, 128),))
    dt_bias = jnp.clip(-4.0 + 4.0 * jax.random.uniform(keys[17], (DI,), jnp.float32) ** shard_levels(keys[17], (DI,), ((0, 128),), -0.2, 0.2), -4.0, 0.0)
    a_log = jnp.clip(2.77 * jax.random.uniform(keys[18], (NSTATE, DI), jnp.float32) ** shard_levels(keys[18], (NSTATE, DI), ((1, 128),), -0.2, 0.2), 0.0, 2.77)
    skip_gain = jnp.clip(0.25 + 1.75 * jax.random.uniform(keys[19], (DI,), jnp.float32) ** shard_levels(keys[19], (DI,), ((0, 128),), -0.2, 0.2), 0.25, 2.0)
    ssm_state = normal_values(own_keys[20], (BATCH_SEQUENCES, NSTATE, DI), 1.0, 6.0, ((0, 2), (2, 128)), jnp.float32)
    w_mamba_out = bell_draw_with(keys[21], (DI, MODEL_DIMENSION), DI ** -0.5, 0.25, ((0, 128),), (0, 1, 128, 5.5))
    return {"tokens": tokens, "attn_gain": attn_gain, "w_query": w_query, "key_projection_weight": key_projection_weight, "value_projection_weight": value_projection_weight, "w_attn_out": w_attn_out, "cache_keys": cache_keys, "stored_value_cache": stored_value_cache, "lengths": lengths, "positions": positions, "mamba_gain": mamba_gain, "w_in": w_in, "conv_weight": conv_weight, "conv_bias": conv_bias, "conv_state": conv_state, "w_xproj": w_xproj, "w_dt": w_dt, "dt_bias": dt_bias, "a_log": a_log, "skip_gain": skip_gain, "ssm_state": ssm_state, "w_mamba_out": w_mamba_out}


norm_eps = 1e-05
rope_base = 10000.0

def apply_rotary(vectors, positions):
    half_dim = vectors.shape[-1] // 2
    frequency = jnp.exp(-math.log(rope_base) * 2.0 * jnp.arange(half_dim, dtype=jnp.float32) / (2 * half_dim))
    angles = positions.astype(jnp.float32)[:, None] * frequency[None, :]
    cosine = jnp.cos(angles)[:, None, :]
    sine_part = jnp.sin(angles)[:, None, :]
    first_half = vectors[..., :half_dim]
    second_half = vectors[..., half_dim:]
    return jnp.concatenate([first_half * cosine - second_half * sine_part, second_half * cosine + first_half * sine_part], axis=-1)

def reference(tokens, attn_gain, w_query, key_projection_weight, value_projection_weight, w_attn_out, cache_keys, stored_value_cache, lengths, positions, mamba_gain, w_in, conv_weight, conv_bias, conv_state, w_xproj, w_dt, dt_bias, a_log, skip_gain, ssm_state, w_mamba_out):
    token_float = tokens.astype(jnp.float32)
    inv_rms = lax.rsqrt(lax.optimization_barrier(jnp.sum(token_float * token_float, axis=1)) / MODEL_DIMENSION + norm_eps)
    lifted = (token_float * attn_gain[None, :]).astype(jnp.bfloat16)
    query_vectors = jnp.dot(lifted, w_query, preferred_element_type=jnp.float32) * inv_rms[:, None]
    fresh_key_rows = jnp.dot(lifted, key_projection_weight, preferred_element_type=jnp.float32) * inv_rms[:, None]
    fresh_value_rows = jnp.dot(lifted, value_projection_weight, preferred_element_type=jnp.float32) * inv_rms[:, None]
    query_vectors = apply_rotary(query_vectors.reshape(BATCH_SEQUENCES, QUERY_HEADS, HEAD_SIZE), positions).astype(jnp.bfloat16)
    fresh_key_rows = apply_rotary(fresh_key_rows.reshape(BATCH_SEQUENCES, KEY_VALUE_HEADS, HEAD_SIZE), positions).astype(jnp.bfloat16)
    fresh_value_rows = fresh_value_rows.reshape(BATCH_SEQUENCES, KEY_VALUE_HEADS, HEAD_SIZE).astype(jnp.bfloat16)
    query_group_count = QUERY_HEADS // KEY_VALUE_HEADS
    grouped_queries = query_vectors.reshape(BATCH_SEQUENCES, KEY_VALUE_HEADS, query_group_count, HEAD_SIZE).astype(jnp.float32)
    score_scale = HEAD_SIZE ** (-0.5)
    scores = jnp.einsum('bhgd,bhtd->bhgt', grouped_queries, cache_keys.astype(jnp.float32)) * score_scale
    score_new = jnp.einsum('bhgd,bhd->bhg', grouped_queries, fresh_key_rows.astype(jnp.float32)) * score_scale
    live_mask = jnp.arange(CACHE_POSITIONS, dtype=jnp.int32)[None, None, None, :] < lengths[:, None, None, None]
    row_max = jnp.maximum(lax.optimization_barrier(jnp.max(jnp.where(live_mask, scores, -jnp.inf), axis=-1)), score_new)
    weights = jnp.where(live_mask, jnp.exp(scores - row_max[..., None]), 0.0)
    new_weight = jnp.exp(score_new - row_max)
    total_weight = lax.optimization_barrier(jnp.sum(weights, axis=-1)) + new_weight
    rounded = lax.optimization_barrier(weights.astype(jnp.bfloat16)).astype(jnp.float32)
    attended = jnp.einsum('bhgt,bhtd->bhgd', rounded, stored_value_cache.astype(jnp.float32))
    attended = attended + new_weight[..., None] * fresh_value_rows.astype(jnp.float32)[:, :, None, :]
    attn_rows = (attended / total_weight[..., None]).reshape(BATCH_SEQUENCES, QUERY_HEADS * HEAD_SIZE).astype(jnp.bfloat16)
    mid_stream = (token_float + jnp.dot(attn_rows, w_attn_out, preferred_element_type=jnp.float32)).astype(jnp.bfloat16)
    mid_float = mid_stream.astype(jnp.float32)
    inv_rms_two = lax.rsqrt(lax.optimization_barrier(jnp.mean(mid_float * mid_float, axis=1)) + norm_eps)
    lifted_two = (mid_float * inv_rms_two[:, None] * mamba_gain[None, :]).astype(jnp.bfloat16)
    inner = jnp.dot(lifted_two, w_in[0], preferred_element_type=jnp.float32)
    gate_branch = jnp.dot(lifted_two, w_in[1], preferred_element_type=jnp.float32)
    window = jnp.concatenate([conv_state, inner[:, None, :]], axis=1)
    mixed = lax.optimization_barrier(jnp.sum(window * conv_weight[None, :, :], axis=1)) + conv_bias[None, :]
    activated = jax.nn.silu(mixed)
    projected = jnp.dot(activated.astype(jnp.bfloat16), w_xproj, preferred_element_type=jnp.float32)
    dt_low = projected[:, :DT_RANK].astype(jnp.bfloat16)
    input_map = projected[:, DT_RANK:DT_RANK + NSTATE]
    output_map = projected[:, DT_RANK + NSTATE:]
    step_size = jax.nn.softplus(jnp.dot(dt_low, w_dt, preferred_element_type=jnp.float32) + dt_bias[None, :])
    decay = jnp.exp(step_size[:, None, :] * (-jnp.exp(a_log))[None, :, :])
    new_state = decay * ssm_state + (step_size * activated)[:, None, :] * input_map[:, :, None]
    readout = lax.optimization_barrier(jnp.sum(output_map[:, :, None] * new_state, axis=1)) + skip_gain[None, :] * activated
    gated = (readout * jax.nn.silu(gate_branch)).astype(jnp.bfloat16)
    hidden_out = (mid_float + jnp.dot(gated, w_mamba_out, preferred_element_type=jnp.float32)).astype(jnp.bfloat16)
    return (hidden_out, new_state)
```

```python
import functools
import math

import jax
import jax.numpy as jnp
import numpy as np
from jax import lax
from jax.experimental import pallas as pl
from jax.experimental.pallas import tpu as pltpu
from jax.sharding import PartitionSpec as P

NORM_EPS = 1e-05
FLOOR = -1e30
ROPE_BASE = 10000.0
MESH = pl.DeviceIdType.MESH
F32 = jnp.float32
BF16 = jnp.bfloat16


def far_first(n):
    return sorted(range(1, n), key=lambda k: -min(k, n - k))


def near_first(n):
    return far_first(n)[::-1]


def dot(a, b):
    return lax.dot_general(a, b, (((1,), (0,)), ((), ())), preferred_element_type=F32)


def dot_t(a, b):
    return lax.dot_general(a, b, (((1,), (1,)), ((), ())), preferred_element_type=F32)


def diagonal(shape):
    return lax.broadcasted_iota(jnp.int32, shape, 0) == lax.broadcasted_iota(jnp.int32, shape, 1)


def column_to_row(column):
    rows = column.shape[0]
    spread = jnp.where(diagonal((rows, 128)), jnp.broadcast_to(column, (rows, 128)), 0.0)
    return jnp.sum(spread, axis=0, keepdims=True)


def row_to_column(row, rows):
    spread = jnp.where(diagonal((rows, row.shape[1])), jnp.broadcast_to(row, (rows, row.shape[1])), 0.0)
    return jnp.sum(spread, axis=1, keepdims=True)


def send_all(axis, n, buffer, send_sem, recv_sem):
    me = lax.axis_index(axis)
    for k in far_first(n):
        pltpu.make_async_remote_copy(
            src_ref=buffer.at[0],
            dst_ref=buffer.at[k],
            send_sem=send_sem,
            recv_sem=recv_sem(k) if callable(recv_sem) else recv_sem,
            device_id={axis: lax.rem(me + k, n)},
            device_id_type=MESH,
        ).start()


def wait_for(buffer, sem, slots):
    part = buffer.at[pl.ds(0, slots)]
    pltpu.make_async_copy(part, part, sem).wait()


def kernel(nz, nx, *refs):
    (
        tokens_h, attn_gain_h, w_query_h, w_key_h, w_value_h, w_out_h, keys_h, values_h, lengths_h, positions_h,
        mamba_gain_h, w_in_h, conv_weight_h, conv_bias_h, conv_state_h, w_xproj_h, w_dt_h, dt_bias_h, a_log_h,
        skip_gain_h, ssm_h, w_mout_h, freq_h,
        hidden_o, state_o,
        tokens, attn_gain, w_query, w_key, w_value, w_out, keys, values, lengths, positions,
        mamba_gain, w_in, conv_weight, conv_bias, conv_state, w_xproj, w_dt, dt_bias, a_log,
        skip_gain, ssm, w_mout, freq,
        load_sem,
        q_buf, below, up_to, total_q, kv_buf, knew, vnew, acc_buf, aux_buf, part_buf, mid_buf, px_buf, pz_buf,
        out_src, share_buf, fin_buf,
        s_q, r_q, s_up, r_up, go, s_kv, r_kv, s_acc, r_acc, s_aux, r_aux, s_part, r_part, s_mid, r_mid,
        s_px, r_px, s_pz, r_pz, s_sh, r_sh, s_fin, r_fin,
    ) = refs
    z = lax.axis_index("seq")
    x = lax.axis_index("head")
    is_owner = z == 0

    loads = {}
    pairs = dict(
        tokens=(tokens_h, tokens), attn_gain=(attn_gain_h, attn_gain), w_query=(w_query_h, w_query), w_key=(w_key_h, w_key),
        w_value=(w_value_h, w_value), positions=(positions_h, positions), freq=(freq_h, freq), lengths=(lengths_h, lengths),
        keys=(keys_h, keys), values=(values_h, values), w_out=(w_out_h, w_out), mamba_gain=(mamba_gain_h, mamba_gain),
        w_in=(w_in_h, w_in), conv_weight=(conv_weight_h, conv_weight), conv_bias=(conv_bias_h, conv_bias),
        conv_state=(conv_state_h, conv_state), w_xproj=(w_xproj_h, w_xproj), w_dt=(w_dt_h, w_dt), dt_bias=(dt_bias_h, dt_bias),
        a_log=(a_log_h, a_log), skip_gain=(skip_gain_h, skip_gain), ssm=(ssm_h, ssm), w_mout=(w_mout_h, w_mout),
    )
    for i, (name, (source, target)) in enumerate(pairs.items()):
        loads[name] = pltpu.make_async_copy(source, target, load_sem.at[i])
        loads[name].start()

    def need(*names):
        for name in names:
            loads.pop(name).wait()

    barrier = pltpu.get_barrier_semaphore()
    for k in far_first(nx):
        pl.semaphore_signal(barrier, inc=1, device_id={"head": lax.rem(x + k, nx)}, device_id_type=MESH)
    pl.semaphore_wait(barrier, nx - 1 + jnp.minimum(z, 1))

    @pl.when(z > 0)
    def _():
        pl.semaphore_signal(go, inc=1, device_id={"seq": z - 1}, device_id_type=MESH)

    @pl.when(z < nz - 1)
    def _():
        pl.semaphore_signal(barrier, inc=1, device_id={"seq": z + 1}, device_id_type=MESH)

    rows = tokens.shape[0]
    feats = tokens.shape[1]
    hd = keys.shape[2]
    span = keys.shape[1]
    groups = w_query.shape[1] // hd
    qrows = groups * rows
    width = feats * nz
    chans = w_xproj.shape[0]
    rank = w_dt.shape[1]
    nstate = a_log.shape[0]

    need("tokens", "attn_gain", "w_query")
    token_f = tokens[...].astype(F32)
    lifted = (token_f * attn_gain[...]).astype(BF16)
    qw = w_query.shape[1]
    q_buf[0, :, :qw] = dot(lifted, w_query[...])
    q_buf[0, :, qw:] = jnp.broadcast_to(jnp.sum(token_f * token_f, axis=1, keepdims=True), (rows, 128))

    for k in far_first(nz):

        @pl.when(z >= k)
        def _(k=k):
            pltpu.make_async_remote_copy(
                src_ref=q_buf.at[0], dst_ref=q_buf.at[k], send_sem=s_q.at[k], recv_sem=r_q.at[k],
                device_id={"seq": z - k}, device_id_type=MESH,
            ).start()

    need("w_key", "w_value")
    kv_buf[0, :, :hd] = dot(lifted, w_key[...])
    kv_buf[0, :, hd:] = dot(lifted, w_value[...])

    @pl.when(z > 0)
    def _():
        pltpu.make_async_remote_copy(
            src_ref=kv_buf.at[0], dst_ref=kv_buf.at[z], send_sem=s_kv, recv_sem=r_kv,
            device_id={"seq": 0}, device_id_type=MESH,
        ).start()

    knew[...] = jnp.zeros_like(knew)
    vnew[...] = jnp.zeros_like(vnew)
    need("positions", "freq", "lengths")
    angle = row_to_column(positions[...].astype(F32), rows) * freq[...]
    cosine = jnp.cos(angle)
    sine = jnp.sin(angle)
    cosine = jnp.concatenate([cosine, cosine], axis=1)
    sine = jnp.concatenate([-sine, sine], axis=1)

    def rotated(v):
        return v * cosine + pltpu.roll(v, hd // 2, 1) * sine

    limit = row_to_column(lengths[...].astype(F32), rows)
    limit = jnp.concatenate([limit] * groups, axis=0)
    spot = (lax.broadcasted_iota(jnp.int32, (qrows, span), 1) + z * span).astype(F32)
    live = spot < limit
    row_of = lax.broadcasted_iota(jnp.int32, (qrows, hd), 0) % rows
    row_of_wide = lax.broadcasted_iota(jnp.int32, (qrows, span), 0) % rows

    up_to[...] = q_buf[0]

    @pl.when(z > 0)
    def _():
        pltpu.make_async_copy(below, below, r_up).wait()
        up_to[...] = q_buf[0] + below[...]

    total_q[...] = up_to[...]

    @pl.when(z < nz - 1)
    def _():
        pl.semaphore_wait(go, 1)
        pltpu.make_async_remote_copy(
            src_ref=up_to, dst_ref=below, send_sem=s_up, recv_sem=r_up, device_id={"seq": z + 1}, device_id_type=MESH,
        ).start()

    for k in range(1, nz):

        @pl.when(z + k < nz)
        def _(k=k):
            pltpu.make_async_copy(q_buf.at[k], q_buf.at[k], r_q.at[k]).wait()
            total_q[...] += q_buf[k]

    r_a = lax.rsqrt(total_q[:, qw:] / width + NORM_EPS)

    @pl.when(is_owner)
    def _():
        wait_for(kv_buf, r_kv, nz - 1)
        kv = kv_buf[0]
        for k in range(1, nz):
            kv = kv + kv_buf[k]
        knew[...] = rotated(kv[:, :hd] * r_a).astype(BF16).astype(F32)
        vnew[...] = (kv[:, hd:] * r_a).astype(BF16).astype(F32)

    q = [rotated(total_q[:, g * hd : (g + 1) * hd] * r_a) for g in range(groups)]
    q = jnp.concatenate(q, axis=0).astype(BF16)

    need("keys")
    scores = jnp.zeros((qrows, span), F32)
    for b in range(rows):
        scores = jnp.where(row_of_wide == b, dot_t(q, keys[b]), scores)
    scale = hd ** (-0.5)
    scores = scores * scale
    top = jnp.max(jnp.where(live, scores, FLOOR), axis=1, keepdims=True)
    fresh = jnp.sum(q.astype(F32) * jnp.concatenate([knew[...]] * groups, axis=0), axis=1, keepdims=True) * scale
    mine = jnp.broadcast_to(is_owner, fresh.shape)
    top = jnp.maximum(top, jnp.where(mine, fresh, FLOOR))
    weights = jnp.where(live, jnp.exp(scores - top), 0.0)
    new_weight = jnp.where(mine, jnp.exp(fresh - top), 0.0)
    total = jnp.sum(weights, axis=1, keepdims=True) + new_weight
    weights = weights.astype(BF16)
    need("values")
    acc = jnp.zeros((qrows, hd), F32)
    for b in range(rows):
        acc = jnp.where(row_of == b, dot(weights, values[b]), acc)
    acc = acc + new_weight * jnp.concatenate([vnew[...]] * groups, axis=0)
    acc_buf[0] = acc.astype(BF16)
    aux_buf[0] = column_to_row(top) + pltpu.roll(column_to_row(total), 64, 1)
    send_all("seq", nz, aux_buf, s_aux, r_aux)
    send_all("seq", nz, acc_buf, s_acc, r_acc)

    need("w_out")
    wait_for(aux_buf, r_aux, nz - 1)
    aux = jnp.concatenate([aux_buf[k] for k in range(nz)], axis=0)
    factor = jnp.exp(aux - jnp.max(aux, axis=0, keepdims=True))
    whole = jnp.sum(factor * pltpu.roll(aux, 64, 1), axis=0, keepdims=True)
    lane = lax.broadcasted_iota(jnp.int32, (nz, 128), 1)
    share = jnp.where(lane < qrows, factor / whole, 0.0)
    share = jnp.concatenate([share, jnp.zeros((128 - nz, 128), F32)], axis=0).T
    wait_for(acc_buf, r_acc, nz - 1)
    attended = share[:qrows, 0:1] * acc_buf[0].astype(F32)
    for k in range(1, nz):
        attended = attended + share[:qrows, k : k + 1] * acc_buf[k].astype(F32)
    attended = jnp.concatenate([attended[g * rows : (g + 1) * rows] for g in range(groups)], axis=1).astype(BF16)
    part_buf[0] = dot(attended, w_out[...]).astype(BF16)
    send_all("head", nx, part_buf, s_part, r_part)
    need("mamba_gain", "w_in")
    wait_for(part_buf, r_part, nx - 1)
    summed = part_buf[lax.rem(x, nx)].astype(F32)
    for j in range(1, nx):
        summed = summed + part_buf[lax.rem(x - j + nx, nx)].astype(F32)
    mid = (token_f + summed).astype(BF16)
    mid_buf[0] = mid
    circle = sorted(range(1, nz), key=lambda k: min(k, nz - k))
    ends = (0, nz // 2, max(nz // 2, nz - 4), nz - 1)
    rings = [circle[i:j] for i, j in zip(ends, ends[1:]) if j > i]
    ring_of = {k: i for i, r in enumerate(rings) for k in r}
    send_all("seq", nz, mid_buf, s_mid, lambda k: r_mid.at[ring_of[k]])

    def block_of(k):
        at = pl.multiple_of(lax.rem(z - k + nz, nz) * feats, feats)
        block = mid_buf[k].astype(F32)
        raised = (block * mamba_gain[:, pl.ds(at, feats)]).astype(BF16)
        return block * block, dot_t(raised, w_in[:, pl.ds(at, feats)])

    squares, both = block_of(0)
    for i, ring in enumerate(rings):
        wait_for(mid_buf, r_mid.at[i], len(ring))
        for k in ring:
            more, extra = block_of(k)
            squares = squares + more
            both = both + extra
    both = both * lax.rsqrt(jnp.sum(squares, axis=1, keepdims=True) / width + NORM_EPS)
    inner = both[:, :chans]
    gate = both[:, chans:]

    need("conv_weight", "conv_bias", "conv_state", "w_xproj")
    mixed = inner * conv_weight[3:4, :] + conv_bias[...]
    for k in range(3):
        mixed = mixed + conv_state[k] * conv_weight[k : k + 1, :]
    u = mixed / (1.0 + jnp.exp(-mixed))
    proj = dot(u.astype(BF16), w_xproj[...])
    px_buf[0] = jnp.concatenate([proj, jnp.zeros((rows, px_buf.shape[2] - proj.shape[1]), F32)], axis=1).astype(BF16)
    send_all("head", nx, px_buf, s_px, r_px)
    need("w_dt", "dt_bias", "a_log", "skip_gain", "ssm", "w_mout")
    decay_rate = -jnp.exp(a_log[...])
    gated = gate / (1.0 + jnp.exp(-gate))
    wait_for(px_buf, r_px, nx - 1)
    proj = px_buf[0].astype(F32)
    for k in range(1, nx):
        proj = proj + px_buf[k].astype(F32)
    pz_buf[0] = proj.astype(BF16)
    send_all("seq", nz, pz_buf, s_pz, r_pz)
    wait_for(pz_buf, r_pz, nz - 1)
    proj = pz_buf[0].astype(F32)
    for k in range(1, nz):
        proj = proj + pz_buf[k].astype(F32)

    pre = dot_t(proj[:, :rank].astype(BF16), w_dt[...]) + dt_bias[...]
    step = jnp.maximum(pre, 0.0) + jnp.log(1.0 + jnp.exp(-jnp.abs(pre)))
    maps = jnp.concatenate([proj[:, rank : rank + 128], jnp.zeros((128 - rows, 128), F32)], axis=0).T
    drive = step * u
    reads = []
    for b in range(rows):
        state = (
            jnp.exp(step[b : b + 1, :] * decay_rate) * ssm[b]
            + drive[b : b + 1, :] * maps[:nstate, b : b + 1]
        )
        state_o[b] = state
        reads.append(jnp.sum(maps[nstate : 2 * nstate, b : b + 1] * state, axis=0, keepdims=True))
    y = (jnp.concatenate(reads, axis=0) + skip_gain[...] * u) * gated
    y = y.astype(BF16)

    def out_block(k):
        at = pl.multiple_of(lax.rem(z + k, nz) * feats, feats)
        return dot(y, w_mout[:, pl.ds(at, feats)]).astype(BF16)

    for k in far_first(nz):
        out_src[k] = out_block(k)
        pltpu.make_async_remote_copy(
            src_ref=out_src.at[k], dst_ref=share_buf.at[k], send_sem=s_sh, recv_sem=r_sh,
            device_id={"seq": lax.rem(z + k, nz)}, device_id_type=MESH,
        ).start()
    result = out_block(0).astype(F32)
    wait_for(share_buf, r_sh, nz - 1)
    for k in range(1, nz):
        result = result + share_buf[k].astype(F32)
    fin_buf[0] = result
    send_all("head", nx, fin_buf, s_fin, r_fin)

    for k in range(1, nz):

        @pl.when(z >= k)
        def _(k=k):
            pltpu.make_async_copy(q_buf.at[0], q_buf.at[0], s_q.at[k]).wait()

    @pl.when(z > 0)
    def _():
        pltpu.make_async_copy(kv_buf.at[0], kv_buf.at[0], s_kv).wait()

    @pl.when(z < nz - 1)
    def _():
        pltpu.make_async_copy(up_to, up_to, s_up).wait()

    wait_for(aux_buf, s_aux, nz - 1)
    wait_for(acc_buf, s_acc, nz - 1)
    wait_for(part_buf, s_part, nx - 1)
    wait_for(mid_buf, s_mid, nz - 1)
    wait_for(px_buf, s_px, nx - 1)
    wait_for(pz_buf, s_pz, nz - 1)
    wait_for(share_buf, s_sh, nz - 1)
    wait_for(fin_buf, r_fin, nx - 1)
    result = fin_buf[lax.rem(x, nx)]
    for j in range(1, nx):
        result = result + fin_buf[lax.rem(x - j + nx, nx)]
    hidden_o[...] = (mid.astype(F32) + result).astype(BF16)
    wait_for(fin_buf, s_fin, nx - 1)


def put_out(hidden, state, hidden_o, state_o, sem):
    copies = [pltpu.make_async_copy(hidden, hidden_o, sem.at[0]), pltpu.make_async_copy(state, state_o, sem.at[1])]
    for copy in copies:
        copy.start()
    for copy in copies:
        copy.wait()


def local(nz, nx, *args):
    (
        tokens, attn_gain, w_query, w_key, w_value, w_out, keys, values, lengths, positions, mamba_gain, w_in,
        conv_weight, conv_bias, conv_state, w_xproj, w_dt, dt_bias, a_log, skip_gain, ssm, w_mout,
    ) = args
    rows, feats = tokens.shape
    hd = keys.shape[3]
    span = keys.shape[2]
    half = hd // 2
    qrows = w_query.shape[1] // hd * rows
    two, width, chans = w_in.shape
    freq = jnp.asarray(np.exp(-math.log(ROPE_BASE) * 2.0 * np.arange(half) / (2 * half)).reshape(1, half), F32)
    operands = (
        tokens, attn_gain.reshape(1, -1), w_query, w_key, w_value, w_out,
        keys.reshape(rows, span, hd), values.reshape(rows, span, hd), lengths.reshape(1, -1), positions.reshape(1, -1),
        mamba_gain.reshape(1, -1), jnp.transpose(w_in, (0, 2, 1)).reshape(two * chans, width),
        conv_weight, conv_bias.reshape(1, -1), jnp.transpose(conv_state, (1, 0, 2)), w_xproj,
        jnp.transpose(w_dt), dt_bias.reshape(1, -1), a_log, skip_gain.reshape(1, -1), ssm, w_mout, freq,
    )
    pad = -(-w_xproj.shape[1] // 128) * 128
    dma = pltpu.SemaphoreType.DMA
    buffers = [
        ((nz, rows, w_query.shape[1] + 128), F32),
        ((rows, w_query.shape[1] + 128), F32),
        ((rows, w_query.shape[1] + 128), F32),
        ((rows, w_query.shape[1] + 128), F32),
        ((nz, rows, 2 * hd), F32),
        ((rows, hd), F32),
        ((rows, hd), F32),
        ((nz, qrows, hd), BF16),
        ((nz, 1, 128), F32),
        ((nx, rows, feats), BF16),
        ((nz, rows, feats), BF16),
        ((nx, rows, pad), BF16),
        ((nz, rows, pad), BF16),
        ((nz, rows, feats), BF16),
        ((nz, rows, feats), BF16),
        ((nx, rows, feats), F32),
    ]
    sems = [dma((nz,)), dma((nz,)), dma, dma, pltpu.SemaphoreType.REGULAR] + [dma] * 8 + [dma, dma((3,))] + [dma] * 8
    hidden, state = pl.pallas_call(
        functools.partial(kernel, nz, nx),
        out_shape=(
            pltpu.VMEM((rows, feats), BF16),
            pltpu.VMEM(ssm.shape, F32),
        ),
        in_specs=[pl.BlockSpec(memory_space=pltpu.HBM)] * len(operands),
        out_specs=(pl.BlockSpec(memory_space=pltpu.VMEM), pl.BlockSpec(memory_space=pltpu.VMEM)),
        scratch_shapes=[pltpu.VMEM(o.shape, o.dtype) for o in operands]
        + [dma((len(operands),))]
        + [pltpu.VMEM(shape, kind) for shape, kind in buffers]
        + sems,
        compiler_params=pltpu.CompilerParams(
            collective_id=0, has_side_effects=True, vmem_limit_bytes=48 * 2**20
        ),
        name="decode_step",
    )(*[pltpu.with_memory_space_constraint(o, pltpu.HBM) for o in operands])
    return pl.pallas_call(
        put_out,
        out_shape=(jax.ShapeDtypeStruct((rows, feats), BF16), jax.ShapeDtypeStruct(ssm.shape, F32)),
        in_specs=[pl.BlockSpec(memory_space=pltpu.VMEM)] * 2,
        out_specs=(pl.BlockSpec(memory_space=pltpu.HBM), pl.BlockSpec(memory_space=pltpu.HBM)),
        scratch_shapes=[dma((2,))],
        name="put_out",
        compiler_params=pltpu.CompilerParams(vmem_limit_bytes=2**20),
    )(*[pltpu.with_memory_space_constraint(o, pltpu.VMEM) for o in (hidden, state)])


def solution(mesh):
    batch = ("rep", "sub")
    chan = ("seq", "head")
    in_specs = (
        P(batch, "seq"), P("seq"), P("seq", "head"), P("seq", "head"), P("seq", "head"), P("head", "seq"),
        P(batch, "head", "seq", None), P(batch, "head", "seq", None), P(batch), P(batch), P(), P(None, None, chan),
        P(None, chan), P(chan), P(batch, None, chan), P(chan, None), P(None, chan), P(chan), P(None, chan), P(chan),
        P(batch, None, chan), P(chan, None),
    )
    out_specs = (P(batch, "seq"), P(batch, None, chan))
    body = functools.partial(local, mesh.shape["seq"], mesh.shape["head"])
    return jax.shard_map(body, mesh=mesh, in_specs=in_specs, out_specs=out_specs, check_vma=False)
```

```python
import functools
import math

import jax
import jax.numpy as jnp
import numpy as np
from jax import lax
from jax.experimental import pallas as pl
from jax.experimental.pallas import tpu as pltpu
from jax.sharding import PartitionSpec as P

NORM_EPS = 1e-05
FLOOR = -1e30
ROPE_BASE = 10000.0
MESH = pl.DeviceIdType.MESH
F32 = jnp.float32
BF16 = jnp.bfloat16


def far_first(n):
    return sorted(range(1, n), key=lambda k: -min(k, n - k))


def near_first(n):
    return far_first(n)[::-1]


def dot(a, b):
    return lax.dot_general(a, b, (((1,), (0,)), ((), ())), preferred_element_type=F32)


def dot_t(a, b):
    return lax.dot_general(a, b, (((1,), (1,)), ((), ())), preferred_element_type=F32)


def diagonal(shape):
    return lax.broadcasted_iota(jnp.int32, shape, 0) == lax.broadcasted_iota(jnp.int32, shape, 1)


def column_to_row(column):
    rows = column.shape[0]
    spread = jnp.where(diagonal((rows, 128)), jnp.broadcast_to(column, (rows, 128)), 0.0)
    return jnp.sum(spread, axis=0, keepdims=True)


def row_to_column(row, rows):
    spread = jnp.where(diagonal((rows, row.shape[1])), jnp.broadcast_to(row, (rows, row.shape[1])), 0.0)
    return jnp.sum(spread, axis=1, keepdims=True)


def send_all(axis, n, buffer, send_sem, recv_sem):
    me = lax.axis_index(axis)
    for k in far_first(n):
        pltpu.make_async_remote_copy(
            src_ref=buffer.at[0],
            dst_ref=buffer.at[k],
            send_sem=send_sem,
            recv_sem=recv_sem(k) if callable(recv_sem) else recv_sem,
            device_id={axis: lax.rem(me + k, n)},
            device_id_type=MESH,
        ).start()


def wait_for(buffer, sem, slots):
    part = buffer.at[pl.ds(0, slots)]
    pltpu.make_async_copy(part, part, sem).wait()


def kernel(nz, nx, *refs):
    (
        tokens_h, attn_gain_h, w_query_h, w_key_h, w_value_h, w_out_h, keys_h, values_h, lengths_h, positions_h,
        mamba_gain_h, w_in_h, conv_weight_h, conv_bias_h, conv_state_h, w_xproj_h, w_dt_h, dt_bias_h, a_log_h,
        skip_gain_h, ssm_h, w_mout_h, freq_h,
        hidden_o, state_o,
        tokens, attn_gain, w_query, w_key, w_value, w_out, keys, values, lengths, positions,
        mamba_gain, w_in, conv_weight, conv_bias, conv_state, w_xproj, w_dt, dt_bias, a_log,
        skip_gain, ssm, w_mout, freq,
        load_sem,
        q_buf, below, up_to, total_q, kv_buf, knew, vnew, acc_buf, aux_buf, part_buf, mid_buf, px_buf, pz_buf,
        out_src, share_buf, fin_buf,
        s_q, r_q, s_up, r_up, go, s_kv, r_kv, s_acc, r_acc, s_aux, r_aux, s_part, r_part, s_mid, r_mid,
        s_px, r_px, s_pz, r_pz, s_sh, r_sh, s_fin, r_fin,
    ) = refs
    z = lax.axis_index("seq")
    x = lax.axis_index("head")
    place = lax.rem(z + nz - 1, nz)
    down, up = lax.rem(z + nz - 1, nz), lax.rem(z + 1, nz)
    is_owner = place == 0

    loads = {}
    pairs = dict(
        tokens=(tokens_h, tokens), attn_gain=(attn_gain_h, attn_gain), w_query=(w_query_h, w_query), w_key=(w_key_h, w_key),
        w_value=(w_value_h, w_value), positions=(positions_h, positions), freq=(freq_h, freq), lengths=(lengths_h, lengths),
        keys=(keys_h, keys), values=(values_h, values), w_out=(w_out_h, w_out), mamba_gain=(mamba_gain_h, mamba_gain),
        w_in=(w_in_h, w_in), conv_weight=(conv_weight_h, conv_weight), conv_bias=(conv_bias_h, conv_bias),
        conv_state=(conv_state_h, conv_state), w_xproj=(w_xproj_h, w_xproj), w_dt=(w_dt_h, w_dt), dt_bias=(dt_bias_h, dt_bias),
        a_log=(a_log_h, a_log), skip_gain=(skip_gain_h, skip_gain), ssm=(ssm_h, ssm), w_mout=(w_mout_h, w_mout),
    )
    for i, (name, (source, target)) in enumerate(pairs.items()):
        loads[name] = pltpu.make_async_copy(source, target, load_sem.at[i])
        loads[name].start()

    def need(*names):
        for name in names:
            loads.pop(name).wait()

    barrier = pltpu.get_barrier_semaphore()
    for k in far_first(nx):
        pl.semaphore_signal(barrier, inc=1, device_id={"head": lax.rem(x + k, nx)}, device_id_type=MESH)
    pl.semaphore_wait(barrier, nx - 1 + jnp.minimum(place, 1))

    @pl.when(place > 0)
    def _():
        pl.semaphore_signal(go, inc=1, device_id={"seq": down}, device_id_type=MESH)

    @pl.when(place < nz - 1)
    def _():
        pl.semaphore_signal(barrier, inc=1, device_id={"seq": up}, device_id_type=MESH)

    rows = tokens.shape[0]
    feats = tokens.shape[1]
    hd = keys.shape[2]
    span = keys.shape[1]
    groups = w_query.shape[1] // hd
    qrows = groups * rows
    width = feats * nz
    chans = w_xproj.shape[0]
    rank = w_dt.shape[1]
    nstate = a_log.shape[0]

    need("tokens", "attn_gain", "w_query")
    token_f = tokens[...].astype(F32)
    lifted = (token_f * attn_gain[...]).astype(BF16)
    qw = w_query.shape[1]
    q_buf[0, :, :qw] = dot(lifted, w_query[...])
    q_buf[0, :, qw:] = jnp.broadcast_to(jnp.sum(token_f * token_f, axis=1, keepdims=True), (rows, 128))

    for k in far_first(nz):

        @pl.when(place >= k)
        def _(k=k):
            pltpu.make_async_remote_copy(
                src_ref=q_buf.at[0], dst_ref=q_buf.at[k], send_sem=s_q.at[k], recv_sem=r_q.at[k],
                device_id={"seq": lax.rem(z + nz - k, nz)}, device_id_type=MESH,
            ).start()

    need("w_key", "w_value")
    kv_buf[0, :, :hd] = dot(lifted, w_key[...])
    kv_buf[0, :, hd:] = dot(lifted, w_value[...])

    @pl.when(place > 0)
    def _():
        pltpu.make_async_remote_copy(
            src_ref=kv_buf.at[0], dst_ref=kv_buf.at[place], send_sem=s_kv, recv_sem=r_kv,
            device_id={"seq": 1}, device_id_type=MESH,
        ).start()

    knew[...] = jnp.zeros_like(knew)
    vnew[...] = jnp.zeros_like(vnew)
    need("positions", "freq", "lengths")
    angle = row_to_column(positions[...].astype(F32), rows) * freq[...]
    cosine = jnp.cos(angle)
    sine = jnp.sin(angle)
    cosine = jnp.concatenate([cosine, cosine], axis=1)
    sine = jnp.concatenate([-sine, sine], axis=1)

    def rotated(v):
        return v * cosine + pltpu.roll(v, hd // 2, 1) * sine

    limit = row_to_column(lengths[...].astype(F32), rows)
    limit = jnp.concatenate([limit] * groups, axis=0)
    spot = (lax.broadcasted_iota(jnp.int32, (qrows, span), 1) + z * span).astype(F32)
    live = spot < limit
    row_of = lax.broadcasted_iota(jnp.int32, (qrows, hd), 0) % rows
    row_of_wide = lax.broadcasted_iota(jnp.int32, (qrows, span), 0) % rows

    up_to[...] = q_buf[0]

    @pl.when(place > 0)
    def _():
        pltpu.make_async_copy(below, below, r_up).wait()
        up_to[...] = q_buf[0] + below[...]

    total_q[...] = up_to[...]

    @pl.when(place < nz - 1)
    def _():
        pl.semaphore_wait(go, 1)
        pltpu.make_async_remote_copy(
            src_ref=up_to, dst_ref=below, send_sem=s_up, recv_sem=r_up, device_id={"seq": up}, device_id_type=MESH,
        ).start()

    for k in range(1, nz):

        @pl.when(place + k < nz)
        def _(k=k):
            pltpu.make_async_copy(q_buf.at[k], q_buf.at[k], r_q.at[k]).wait()
            total_q[...] += q_buf[k]

    r_a = lax.rsqrt(total_q[:, qw:] / width + NORM_EPS)

    @pl.when(is_owner)
    def _():
        wait_for(kv_buf, r_kv, nz - 1)
        kv = kv_buf[0]
        for k in range(1, nz):
            kv = kv + kv_buf[k]
        knew[...] = rotated(kv[:, :hd] * r_a).astype(BF16).astype(F32)
        vnew[...] = (kv[:, hd:] * r_a).astype(BF16).astype(F32)

    q = [rotated(total_q[:, g * hd : (g + 1) * hd] * r_a) for g in range(groups)]
    q = jnp.concatenate(q, axis=0).astype(BF16)

    need("keys")
    scores = jnp.zeros((qrows, span), F32)
    for b in range(rows):
        scores = jnp.where(row_of_wide == b, dot_t(q, keys[b]), scores)
    scale = hd ** (-0.5)
    scores = scores * scale
    top = jnp.max(jnp.where(live, scores, FLOOR), axis=1, keepdims=True)
    fresh = jnp.sum(q.astype(F32) * jnp.concatenate([knew[...]] * groups, axis=0), axis=1, keepdims=True) * scale
    mine = jnp.broadcast_to(is_owner, fresh.shape)
    top = jnp.maximum(top, jnp.where(mine, fresh, FLOOR))
    weights = jnp.where(live, jnp.exp(scores - top), 0.0)
    new_weight = jnp.where(mine, jnp.exp(fresh - top), 0.0)
    total = jnp.sum(weights, axis=1, keepdims=True) + new_weight
    weights = weights.astype(BF16)
    need("values")
    acc = jnp.zeros((qrows, hd), F32)
    for b in range(rows):
        acc = jnp.where(row_of == b, dot(weights, values[b]), acc)
    acc = acc + new_weight * jnp.concatenate([vnew[...]] * groups, axis=0)
    acc_buf[0] = acc.astype(BF16)
    aux_buf[0] = column_to_row(top) + pltpu.roll(column_to_row(total), 64, 1)
    send_all("seq", nz, aux_buf, s_aux, r_aux)
    send_all("seq", nz, acc_buf, s_acc, r_acc)

    need("w_out")
    wait_for(aux_buf, r_aux, nz - 1)
    aux = jnp.concatenate([aux_buf[k] for k in range(nz)], axis=0)
    factor = jnp.exp(aux - jnp.max(aux, axis=0, keepdims=True))
    whole = jnp.sum(factor * pltpu.roll(aux, 64, 1), axis=0, keepdims=True)
    lane = lax.broadcasted_iota(jnp.int32, (nz, 128), 1)
    share = jnp.where(lane < qrows, factor / whole, 0.0)
    share = jnp.concatenate([share, jnp.zeros((128 - nz, 128), F32)], axis=0).T
    wait_for(acc_buf, r_acc, nz - 1)
    attended = share[:qrows, 0:1] * acc_buf[0].astype(F32)
    for k in range(1, nz):
        attended = attended + share[:qrows, k : k + 1] * acc_buf[k].astype(F32)
    attended = jnp.concatenate([attended[g * rows : (g + 1) * rows] for g in range(groups)], axis=1).astype(BF16)
    part_buf[0] = dot(attended, w_out[...]).astype(BF16)
    send_all("head", nx, part_buf, s_part, r_part)
    need("mamba_gain", "w_in")
    wait_for(part_buf, r_part, nx - 1)
    summed = part_buf[lax.rem(x, nx)].astype(F32)
    for j in range(1, nx):
        summed = summed + part_buf[lax.rem(x - j + nx, nx)].astype(F32)
    mid = (token_f + summed).astype(BF16)
    mid_buf[0] = mid
    circle = sorted(range(1, nz), key=lambda k: min(k, nz - k))
    ends = (0, nz // 2, max(nz // 2, nz - 4), nz - 1)
    rings = [circle[i:j] for i, j in zip(ends, ends[1:]) if j > i]
    ring_of = {k: i for i, r in enumerate(rings) for k in r}
    send_all("seq", nz, mid_buf, s_mid, lambda k: r_mid.at[ring_of[k]])

    def block_of(k):
        at = pl.multiple_of(lax.rem(z - k + nz, nz) * feats, feats)
        block = mid_buf[k].astype(F32)
        raised = (block * mamba_gain[:, pl.ds(at, feats)]).astype(BF16)
        return block * block, dot_t(raised, w_in[:, pl.ds(at, feats)])

    squares, both = block_of(0)
    for i, ring in enumerate(rings):
        wait_for(mid_buf, r_mid.at[i], len(ring))
        for k in ring:
            more, extra = block_of(k)
            squares = squares + more
            both = both + extra
    both = both * lax.rsqrt(jnp.sum(squares, axis=1, keepdims=True) / width + NORM_EPS)
    inner = both[:, :chans]
    gate = both[:, chans:]

    need("conv_weight", "conv_bias", "conv_state", "w_xproj")
    mixed = inner * conv_weight[3:4, :] + conv_bias[...]
    for k in range(3):
        mixed = mixed + conv_state[k] * conv_weight[k : k + 1, :]
    u = mixed / (1.0 + jnp.exp(-mixed))
    proj = dot(u.astype(BF16), w_xproj[...])
    px_buf[0] = jnp.concatenate([proj, jnp.zeros((rows, px_buf.shape[2] - proj.shape[1]), F32)], axis=1).astype(BF16)
    send_all("head", nx, px_buf, s_px, r_px)
    need("w_dt", "dt_bias", "a_log", "skip_gain", "ssm", "w_mout")
    decay_rate = -jnp.exp(a_log[...])
    gated = gate / (1.0 + jnp.exp(-gate))
    wait_for(px_buf, r_px, nx - 1)
    proj = px_buf[0].astype(F32)
    for k in range(1, nx):
        proj = proj + px_buf[k].astype(F32)
    pz_buf[0] = proj.astype(BF16)
    send_all("seq", nz, pz_buf, s_pz, r_pz)
    wait_for(pz_buf, r_pz, nz - 1)
    proj = pz_buf[0].astype(F32)
    for k in range(1, nz):
        proj = proj + pz_buf[k].astype(F32)

    pre = dot_t(proj[:, :rank].astype(BF16), w_dt[...]) + dt_bias[...]
    step = jnp.maximum(pre, 0.0) + jnp.log(1.0 + jnp.exp(-jnp.abs(pre)))
    maps = jnp.concatenate([proj[:, rank : rank + 128], jnp.zeros((128 - rows, 128), F32)], axis=0).T
    drive = step * u
    reads = []
    for b in range(rows):
        state = (
            jnp.exp(step[b : b + 1, :] * decay_rate) * ssm[b]
            + drive[b : b + 1, :] * maps[:nstate, b : b + 1]
        )
        state_o[b] = state
        reads.append(jnp.sum(maps[nstate : 2 * nstate, b : b + 1] * state, axis=0, keepdims=True))
    y = (jnp.concatenate(reads, axis=0) + skip_gain[...] * u) * gated
    y = y.astype(BF16)

    def out_block(k):
        at = pl.multiple_of(lax.rem(z + k, nz) * feats, feats)
        return dot(y, w_mout[:, pl.ds(at, feats)]).astype(BF16)

    for k in far_first(nz):
        out_src[k] = out_block(k)
        pltpu.make_async_remote_copy(
            src_ref=out_src.at[k], dst_ref=share_buf.at[k], send_sem=s_sh, recv_sem=r_sh,
            device_id={"seq": lax.rem(z + k, nz)}, device_id_type=MESH,
        ).start()
    result = out_block(0).astype(F32)
    wait_for(share_buf, r_sh, nz - 1)
    for k in range(1, nz):
        result = result + share_buf[k].astype(F32)
    fin_buf[0] = result
    send_all("head", nx, fin_buf, s_fin, r_fin)

    for k in range(1, nz):

        @pl.when(place >= k)
        def _(k=k):
            pltpu.make_async_copy(q_buf.at[0], q_buf.at[0], s_q.at[k]).wait()

    @pl.when(place > 0)
    def _():
        pltpu.make_async_copy(kv_buf.at[0], kv_buf.at[0], s_kv).wait()

    @pl.when(place < nz - 1)
    def _():
        pltpu.make_async_copy(up_to, up_to, s_up).wait()

    wait_for(aux_buf, s_aux, nz - 1)
    wait_for(acc_buf, s_acc, nz - 1)
    wait_for(part_buf, s_part, nx - 1)
    wait_for(mid_buf, s_mid, nz - 1)
    wait_for(px_buf, s_px, nx - 1)
    wait_for(pz_buf, s_pz, nz - 1)
    wait_for(share_buf, s_sh, nz - 1)
    wait_for(fin_buf, r_fin, nx - 1)
    result = fin_buf[lax.rem(x, nx)]
    for j in range(1, nx):
        result = result + fin_buf[lax.rem(x - j + nx, nx)]
    hidden_o[...] = (mid.astype(F32) + result).astype(BF16)
    wait_for(fin_buf, s_fin, nx - 1)


def put_out(hidden, state, hidden_o, state_o, sem):
    copies = [pltpu.make_async_copy(hidden, hidden_o, sem.at[0]), pltpu.make_async_copy(state, state_o, sem.at[1])]
    for copy in copies:
        copy.start()
    for copy in copies:
        copy.wait()


def local(nz, nx, *args):
    (
        tokens, attn_gain, w_query, w_key, w_value, w_out, keys, values, lengths, positions, mamba_gain, w_in,
        conv_weight, conv_bias, conv_state, w_xproj, w_dt, dt_bias, a_log, skip_gain, ssm, w_mout,
    ) = args
    rows, feats = tokens.shape
    hd = keys.shape[3]
    span = keys.shape[2]
    half = hd // 2
    qrows = w_query.shape[1] // hd * rows
    two, width, chans = w_in.shape
    freq = jnp.asarray(np.exp(-math.log(ROPE_BASE) * 2.0 * np.arange(half) / (2 * half)).reshape(1, half), F32)
    operands = (
        tokens, attn_gain.reshape(1, -1), w_query, w_key, w_value, w_out,
        keys.reshape(rows, span, hd), values.reshape(rows, span, hd), lengths.reshape(1, -1), positions.reshape(1, -1),
        mamba_gain.reshape(1, -1), jnp.transpose(w_in, (0, 2, 1)).reshape(two * chans, width),
        conv_weight, conv_bias.reshape(1, -1), jnp.transpose(conv_state, (1, 0, 2)), w_xproj,
        jnp.transpose(w_dt), dt_bias.reshape(1, -1), a_log, skip_gain.reshape(1, -1), ssm, w_mout, freq,
    )
    pad = -(-w_xproj.shape[1] // 128) * 128
    dma = pltpu.SemaphoreType.DMA
    buffers = [
        ((nz, rows, w_query.shape[1] + 128), F32),
        ((rows, w_query.shape[1] + 128), F32),
        ((rows, w_query.shape[1] + 128), F32),
        ((rows, w_query.shape[1] + 128), F32),
        ((nz, rows, 2 * hd), F32),
        ((rows, hd), F32),
        ((rows, hd), F32),
        ((nz, qrows, hd), BF16),
        ((nz, 1, 128), F32),
        ((nx, rows, feats), BF16),
        ((nz, rows, feats), BF16),
        ((nx, rows, pad), BF16),
        ((nz, rows, pad), BF16),
        ((nz, rows, feats), BF16),
        ((nz, rows, feats), BF16),
        ((nx, rows, feats), F32),
    ]
    sems = [dma((nz,)), dma((nz,)), dma, dma, pltpu.SemaphoreType.REGULAR] + [dma] * 8 + [dma, dma((3,))] + [dma] * 8
    hidden, state = pl.pallas_call(
        functools.partial(kernel, nz, nx),
        out_shape=(
            pltpu.VMEM((rows, feats), BF16),
            pltpu.VMEM(ssm.shape, F32),
        ),
        in_specs=[pl.BlockSpec(memory_space=pltpu.HBM)] * len(operands),
        out_specs=(pl.BlockSpec(memory_space=pltpu.VMEM), pl.BlockSpec(memory_space=pltpu.VMEM)),
        scratch_shapes=[pltpu.VMEM(o.shape, o.dtype) for o in operands]
        + [dma((len(operands),))]
        + [pltpu.VMEM(shape, kind) for shape, kind in buffers]
        + sems,
        compiler_params=pltpu.CompilerParams(
            collective_id=0, has_side_effects=True, vmem_limit_bytes=48 * 2**20
        ),
        name="decode_step",
    )(*[pltpu.with_memory_space_constraint(o, pltpu.HBM) for o in operands])
    return pl.pallas_call(
        put_out,
        out_shape=(jax.ShapeDtypeStruct((rows, feats), BF16), jax.ShapeDtypeStruct(ssm.shape, F32)),
        in_specs=[pl.BlockSpec(memory_space=pltpu.VMEM)] * 2,
        out_specs=(pl.BlockSpec(memory_space=pltpu.HBM), pl.BlockSpec(memory_space=pltpu.HBM)),
        scratch_shapes=[dma((2,))],
        name="put_out",
        compiler_params=pltpu.CompilerParams(vmem_limit_bytes=2**20),
    )(*[pltpu.with_memory_space_constraint(o, pltpu.VMEM) for o in (hidden, state)])


def solution(mesh):
    batch = ("rep", "sub")
    chan = ("seq", "head")
    in_specs = (
        P(batch, "seq"), P("seq"), P("seq", "head"), P("seq", "head"), P("seq", "head"), P("head", "seq"),
        P(batch, "head", "seq", None), P(batch, "head", "seq", None), P(batch), P(batch), P(), P(None, None, chan),
        P(None, chan), P(chan), P(batch, None, chan), P(chan, None), P(None, chan), P(chan), P(None, chan), P(chan),
        P(batch, None, chan), P(chan, None),
    )
    out_specs = (P(batch, "seq"), P(batch, None, chan))
    body = functools.partial(local, mesh.shape["seq"], mesh.shape["head"])
    return jax.shard_map(body, mesh=mesh, in_specs=in_specs, out_specs=out_specs, check_vma=False)
```

```python
import functools
import math

import jax
import jax.numpy as jnp
import numpy as np
from jax import lax
from jax.experimental import pallas as pl
from jax.experimental.pallas import tpu as pltpu
from jax.sharding import PartitionSpec as P

NORM_EPS = 1e-05
FLOOR = -1e30
ROPE_BASE = 10000.0
MESH = pl.DeviceIdType.MESH
F32 = jnp.float32
BF16 = jnp.bfloat16


def far_first(n):
    return sorted(range(1, n), key=lambda k: -min(k, n - k))


def near_first(n):
    return far_first(n)[::-1]


def dot(a, b):
    return lax.dot_general(a, b, (((1,), (0,)), ((), ())), preferred_element_type=F32)


def dot_t(a, b):
    return lax.dot_general(a, b, (((1,), (1,)), ((), ())), preferred_element_type=F32)


def diagonal(shape):
    return lax.broadcasted_iota(jnp.int32, shape, 0) == lax.broadcasted_iota(jnp.int32, shape, 1)


def column_to_row(column):
    rows = column.shape[0]
    spread = jnp.where(diagonal((rows, 128)), jnp.broadcast_to(column, (rows, 128)), 0.0)
    return jnp.sum(spread, axis=0, keepdims=True)


def row_to_column(row, rows):
    spread = jnp.where(diagonal((rows, row.shape[1])), jnp.broadcast_to(row, (rows, row.shape[1])), 0.0)
    return jnp.sum(spread, axis=1, keepdims=True)


def send_all(axis, n, buffer, send_sem, recv_sem):
    me = lax.axis_index(axis)
    for k in far_first(n):
        pltpu.make_async_remote_copy(
            src_ref=buffer.at[0],
            dst_ref=buffer.at[k],
            send_sem=send_sem,
            recv_sem=recv_sem(k) if callable(recv_sem) else recv_sem,
            device_id={axis: lax.rem(me + k, n)},
            device_id_type=MESH,
        ).start()


def wait_for(buffer, sem, slots):
    part = buffer.at[pl.ds(0, slots)]
    pltpu.make_async_copy(part, part, sem).wait()


def kernel(nz, nx, *refs):
    (
        tokens_h, attn_gain_h, w_query_h, w_key_h, w_value_h, w_out_h, keys_h, values_h, lengths_h, positions_h,
        mamba_gain_h, w_in_h, conv_weight_h, conv_bias_h, conv_state_h, w_xproj_h, w_dt_h, dt_bias_h, a_log_h,
        skip_gain_h, ssm_h, w_mout_h, freq_h,
        hidden_o, state_o,
        tokens, attn_gain, w_query, w_key, w_value, w_out, keys, values, lengths, positions,
        mamba_gain, w_in, conv_weight, conv_bias, conv_state, w_xproj, w_dt, dt_bias, a_log,
        skip_gain, ssm, w_mout, freq,
        load_sem,
        q_buf, below, up_to, total_q, kv_buf, knew, vnew, acc_buf, aux_buf, part_buf, mid_buf, px_buf, pz_buf,
        out_src, share_buf, fin_buf,
        s_q, r_q, s_up, r_up, go, ready_x, ready, s_kv, r_kv, s_acc, r_acc, s_aux, r_aux, s_part, r_part, s_mid, r_mid,
        s_px, r_px, s_pz, r_pz, s_sh, r_sh, s_fin, r_fin,
    ) = refs
    z = lax.axis_index("seq")
    x = lax.axis_index("head")
    place = lax.rem(z + nz - 1, nz)
    up = lax.rem(z + 1, nz)
    is_owner = place == 0

    loads = {}
    pairs = dict(
        tokens=(tokens_h, tokens), attn_gain=(attn_gain_h, attn_gain), w_query=(w_query_h, w_query), w_key=(w_key_h, w_key),
        w_value=(w_value_h, w_value), positions=(positions_h, positions), freq=(freq_h, freq), lengths=(lengths_h, lengths),
        keys=(keys_h, keys), values=(values_h, values), w_out=(w_out_h, w_out), mamba_gain=(mamba_gain_h, mamba_gain),
        w_in=(w_in_h, w_in), conv_weight=(conv_weight_h, conv_weight), conv_bias=(conv_bias_h, conv_bias),
        conv_state=(conv_state_h, conv_state), w_xproj=(w_xproj_h, w_xproj), w_dt=(w_dt_h, w_dt), dt_bias=(dt_bias_h, dt_bias),
        a_log=(a_log_h, a_log), skip_gain=(skip_gain_h, skip_gain), ssm=(ssm_h, ssm), w_mout=(w_mout_h, w_mout),
    )
    for i, (name, (source, target)) in enumerate(pairs.items()):
        loads[name] = pltpu.make_async_copy(source, target, load_sem.at[i])
        loads[name].start()

    def need(*names):
        for name in names:
            loads.pop(name).wait()

    barrier = pltpu.get_barrier_semaphore()

    @pl.when(place == 0)
    def _():
        for k in far_first(nx):
            pl.semaphore_signal(barrier, inc=1, device_id={"head": lax.rem(x + k, nx)}, device_id_type=MESH)

    pl.semaphore_wait(barrier, jnp.where(place == 0, nx - 1, 1))

    @pl.when(place < nz - 1)
    def _():
        pl.semaphore_signal(barrier, inc=1, device_id={"seq": up}, device_id_type=MESH)

    for i in (1, 2):

        @pl.when(place >= i)
        def _(i=i):
            pl.semaphore_signal(go.at[i], inc=1, device_id={"seq": lax.rem(z + nz - i, nz)}, device_id_type=MESH)

    rows = tokens.shape[0]
    feats = tokens.shape[1]
    hd = keys.shape[2]
    span = keys.shape[1]
    groups = w_query.shape[1] // hd
    qrows = groups * rows
    width = feats * nz
    chans = w_xproj.shape[0]
    rank = w_dt.shape[1]
    nstate = a_log.shape[0]

    need("tokens", "attn_gain", "w_query")
    token_f = tokens[...].astype(F32)
    lifted = (token_f * attn_gain[...]).astype(BF16)
    qw = w_query.shape[1]
    q_buf[0, :, :qw] = dot(lifted, w_query[...])
    q_buf[0, :, qw:] = jnp.broadcast_to(jnp.sum(token_f * token_f, axis=1, keepdims=True), (rows, 128))

    for k in far_first(nz):

        @pl.when(place >= k)
        def _(k=k):
            pltpu.make_async_remote_copy(
                src_ref=q_buf.at[0], dst_ref=q_buf.at[k], send_sem=s_q.at[k], recv_sem=r_q.at[k],
                device_id={"seq": lax.rem(z + nz - k, nz)}, device_id_type=MESH,
            ).start()

    need("w_key", "w_value")
    kv_buf[0, :, :hd] = dot(lifted, w_key[...])
    kv_buf[0, :, hd:] = dot(lifted, w_value[...])

    @pl.when(place > 0)
    def _():
        pltpu.make_async_remote_copy(
            src_ref=kv_buf.at[0], dst_ref=kv_buf.at[place], send_sem=s_kv, recv_sem=r_kv,
            device_id={"seq": 1}, device_id_type=MESH,
        ).start()

    knew[...] = jnp.zeros_like(knew)
    vnew[...] = jnp.zeros_like(vnew)
    need("positions", "freq", "lengths")
    angle = row_to_column(positions[...].astype(F32), rows) * freq[...]
    cosine = jnp.cos(angle)
    sine = jnp.sin(angle)
    cosine = jnp.concatenate([cosine, cosine], axis=1)
    sine = jnp.concatenate([-sine, sine], axis=1)

    def rotated(v):
        return v * cosine + pltpu.roll(v, hd // 2, 1) * sine

    limit = row_to_column(lengths[...].astype(F32), rows)
    limit = jnp.concatenate([limit] * groups, axis=0)
    spot = (lax.broadcasted_iota(jnp.int32, (qrows, span), 1) + z * span).astype(F32)
    live = spot < limit
    row_of = lax.broadcasted_iota(jnp.int32, (qrows, hd), 0) % rows
    row_of_wide = lax.broadcasted_iota(jnp.int32, (qrows, span), 0) % rows

    up_to[...] = q_buf[0]

    @pl.when(place >= 2)
    def _():
        pltpu.make_async_copy(below.at[1], below.at[1], r_up.at[1]).wait()
        up_to[...] = q_buf[0] + below[1]

    total_q[...] = up_to[...]

    for i in (1, 2):

        @pl.when(place < nz - i)
        def _(i=i):
            pl.semaphore_wait(go.at[i], 1)
            pltpu.make_async_remote_copy(
                src_ref=up_to, dst_ref=below.at[i - 1], send_sem=s_up.at[i - 1], recv_sem=r_up.at[i - 1],
                device_id={"seq": lax.rem(z + i, nz)}, device_id_type=MESH,
            ).start()

    @pl.when(place >= 1)
    def _():
        pltpu.make_async_copy(below.at[0], below.at[0], r_up.at[0]).wait()
        total_q[...] += below[0]

    for k in range(1, nz):

        @pl.when(place + k < nz)
        def _(k=k):
            pltpu.make_async_copy(q_buf.at[k], q_buf.at[k], r_q.at[k]).wait()
            total_q[...] += q_buf[k]

    @pl.when(place == 0)
    def _():
        for k in far_first(nx):
            pl.semaphore_signal(ready_x, inc=1, device_id={"head": lax.rem(x + k, nx)}, device_id_type=MESH)

    r_a = lax.rsqrt(total_q[:, qw:] / width + NORM_EPS)

    @pl.when(is_owner)
    def _():
        wait_for(kv_buf, r_kv, nz - 1)
        kv = kv_buf[0]
        for k in range(1, nz):
            kv = kv + kv_buf[k]
        knew[...] = rotated(kv[:, :hd] * r_a).astype(BF16).astype(F32)
        vnew[...] = (kv[:, hd:] * r_a).astype(BF16).astype(F32)

    q = [rotated(total_q[:, g * hd : (g + 1) * hd] * r_a) for g in range(groups)]
    q = jnp.concatenate(q, axis=0).astype(BF16)

    need("keys")
    scores = jnp.zeros((qrows, span), F32)
    for b in range(rows):
        scores = jnp.where(row_of_wide == b, dot_t(q, keys[b]), scores)
    scale = hd ** (-0.5)
    scores = scores * scale
    top = jnp.max(jnp.where(live, scores, FLOOR), axis=1, keepdims=True)
    fresh = jnp.sum(q.astype(F32) * jnp.concatenate([knew[...]] * groups, axis=0), axis=1, keepdims=True) * scale
    mine = jnp.broadcast_to(is_owner, fresh.shape)
    top = jnp.maximum(top, jnp.where(mine, fresh, FLOOR))
    weights = jnp.where(live, jnp.exp(scores - top), 0.0)
    new_weight = jnp.where(mine, jnp.exp(fresh - top), 0.0)
    total = jnp.sum(weights, axis=1, keepdims=True) + new_weight
    weights = weights.astype(BF16)
    need("values")
    acc = jnp.zeros((qrows, hd), F32)
    for b in range(rows):
        acc = jnp.where(row_of == b, dot(weights, values[b]), acc)
    acc = acc + new_weight * jnp.concatenate([vnew[...]] * groups, axis=0)
    acc_buf[0] = acc.astype(BF16)
    aux_buf[0] = column_to_row(top) + pltpu.roll(column_to_row(total), 64, 1)
    send_all("seq", nz, aux_buf, s_aux, r_aux)
    send_all("seq", nz, acc_buf, s_acc, r_acc)

    @pl.when(place == 0)
    def _():
        pl.semaphore_wait(ready_x, nx - 1)
        for k in far_first(nz):
            pl.semaphore_signal(ready, inc=1, device_id={"seq": lax.rem(z + k, nz)}, device_id_type=MESH)


    need("w_out")
    wait_for(aux_buf, r_aux, nz - 1)
    aux = jnp.concatenate([aux_buf[k] for k in range(nz)], axis=0)
    factor = jnp.exp(aux - jnp.max(aux, axis=0, keepdims=True))
    whole = jnp.sum(factor * pltpu.roll(aux, 64, 1), axis=0, keepdims=True)
    lane = lax.broadcasted_iota(jnp.int32, (nz, 128), 1)
    share = jnp.where(lane < qrows, factor / whole, 0.0)
    share = jnp.concatenate([share, jnp.zeros((128 - nz, 128), F32)], axis=0).T
    wait_for(acc_buf, r_acc, nz - 1)
    attended = share[:qrows, 0:1] * acc_buf[0].astype(F32)
    for k in range(1, nz):
        attended = attended + share[:qrows, k : k + 1] * acc_buf[k].astype(F32)
    attended = jnp.concatenate([attended[g * rows : (g + 1) * rows] for g in range(groups)], axis=1).astype(BF16)
    part_buf[0] = dot(attended, w_out[...]).astype(BF16)

    @pl.when(place > 0)
    def _():
        pl.semaphore_wait(ready, 1)

    send_all("head", nx, part_buf, s_part, r_part)
    need("mamba_gain", "w_in")
    wait_for(part_buf, r_part, nx - 1)
    summed = part_buf[lax.rem(x, nx)].astype(F32)
    for j in range(1, nx):
        summed = summed + part_buf[lax.rem(x - j + nx, nx)].astype(F32)
    mid = (token_f + summed).astype(BF16)
    mid_buf[0] = mid
    circle = sorted(range(1, nz), key=lambda k: min(k, nz - k))
    ends = (0, nz // 2, max(nz // 2, nz - 4), nz - 1)
    rings = [circle[i:j] for i, j in zip(ends, ends[1:]) if j > i]
    ring_of = {k: i for i, r in enumerate(rings) for k in r}
    send_all("seq", nz, mid_buf, s_mid, lambda k: r_mid.at[ring_of[k]])

    def block_of(k):
        at = pl.multiple_of(lax.rem(z - k + nz, nz) * feats, feats)
        block = mid_buf[k].astype(F32)
        raised = (block * mamba_gain[:, pl.ds(at, feats)]).astype(BF16)
        return block * block, dot_t(raised, w_in[:, pl.ds(at, feats)])

    squares, both = block_of(0)
    for i, ring in enumerate(rings):
        wait_for(mid_buf, r_mid.at[i], len(ring))
        for k in ring:
            more, extra = block_of(k)
            squares = squares + more
            both = both + extra
    both = both * lax.rsqrt(jnp.sum(squares, axis=1, keepdims=True) / width + NORM_EPS)
    inner = both[:, :chans]
    gate = both[:, chans:]

    need("conv_weight", "conv_bias", "conv_state", "w_xproj")
    mixed = inner * conv_weight[3:4, :] + conv_bias[...]
    for k in range(3):
        mixed = mixed + conv_state[k] * conv_weight[k : k + 1, :]
    u = mixed / (1.0 + jnp.exp(-mixed))
    proj = dot(u.astype(BF16), w_xproj[...])
    px_buf[0] = jnp.concatenate([proj, jnp.zeros((rows, px_buf.shape[2] - proj.shape[1]), F32)], axis=1).astype(BF16)
    send_all("head", nx, px_buf, s_px, r_px)
    need("w_dt", "dt_bias", "a_log", "skip_gain", "ssm", "w_mout")
    decay_rate = -jnp.exp(a_log[...])
    gated = gate / (1.0 + jnp.exp(-gate))
    wait_for(px_buf, r_px, nx - 1)
    proj = px_buf[0].astype(F32)
    for k in range(1, nx):
        proj = proj + px_buf[k].astype(F32)
    pz_buf[0] = proj.astype(BF16)
    send_all("seq", nz, pz_buf, s_pz, r_pz)
    wait_for(pz_buf, r_pz, nz - 1)
    proj = pz_buf[0].astype(F32)
    for k in range(1, nz):
        proj = proj + pz_buf[k].astype(F32)

    pre = dot_t(proj[:, :rank].astype(BF16), w_dt[...]) + dt_bias[...]
    step = jnp.maximum(pre, 0.0) + jnp.log(1.0 + jnp.exp(-jnp.abs(pre)))
    maps = jnp.concatenate([proj[:, rank : rank + 128], jnp.zeros((128 - rows, 128), F32)], axis=0).T
    drive = step * u
    reads = []
    for b in range(rows):
        state = (
            jnp.exp(step[b : b + 1, :] * decay_rate) * ssm[b]
            + drive[b : b + 1, :] * maps[:nstate, b : b + 1]
        )
        state_o[b] = state
        reads.append(jnp.sum(maps[nstate : 2 * nstate, b : b + 1] * state, axis=0, keepdims=True))
    y = (jnp.concatenate(reads, axis=0) + skip_gain[...] * u) * gated
    y = y.astype(BF16)

    def out_block(k):
        at = pl.multiple_of(lax.rem(z + k, nz) * feats, feats)
        return dot(y, w_mout[:, pl.ds(at, feats)]).astype(BF16)

    for k in far_first(nz):
        out_src[k] = out_block(k)
        pltpu.make_async_remote_copy(
            src_ref=out_src.at[k], dst_ref=share_buf.at[k], send_sem=s_sh, recv_sem=r_sh,
            device_id={"seq": lax.rem(z + k, nz)}, device_id_type=MESH,
        ).start()
    result = out_block(0).astype(F32)
    wait_for(share_buf, r_sh, nz - 1)
    for k in range(1, nz):
        result = result + share_buf[k].astype(F32)
    fin_buf[0] = result
    send_all("head", nx, fin_buf, s_fin, r_fin)

    for k in range(1, nz):

        @pl.when(place >= k)
        def _(k=k):
            pltpu.make_async_copy(q_buf.at[0], q_buf.at[0], s_q.at[k]).wait()

    @pl.when(place > 0)
    def _():
        pltpu.make_async_copy(kv_buf.at[0], kv_buf.at[0], s_kv).wait()

    for i in (1, 2):

        @pl.when(place < nz - i)
        def _(i=i):
            pltpu.make_async_copy(up_to, up_to, s_up.at[i - 1]).wait()

    wait_for(aux_buf, s_aux, nz - 1)
    wait_for(acc_buf, s_acc, nz - 1)
    wait_for(part_buf, s_part, nx - 1)
    wait_for(mid_buf, s_mid, nz - 1)
    wait_for(px_buf, s_px, nx - 1)
    wait_for(pz_buf, s_pz, nz - 1)
    wait_for(share_buf, s_sh, nz - 1)
    wait_for(fin_buf, r_fin, nx - 1)
    result = fin_buf[lax.rem(x, nx)]
    for j in range(1, nx):
        result = result + fin_buf[lax.rem(x - j + nx, nx)]
    hidden_o[...] = (mid.astype(F32) + result).astype(BF16)
    wait_for(fin_buf, s_fin, nx - 1)


def put_out(hidden, state, hidden_o, state_o, sem):
    copies = [pltpu.make_async_copy(hidden, hidden_o, sem.at[0]), pltpu.make_async_copy(state, state_o, sem.at[1])]
    for copy in copies:
        copy.start()
    for copy in copies:
        copy.wait()


def local(nz, nx, *args):
    (
        tokens, attn_gain, w_query, w_key, w_value, w_out, keys, values, lengths, positions, mamba_gain, w_in,
        conv_weight, conv_bias, conv_state, w_xproj, w_dt, dt_bias, a_log, skip_gain, ssm, w_mout,
    ) = args
    rows, feats = tokens.shape
    hd = keys.shape[3]
    span = keys.shape[2]
    half = hd // 2
    qrows = w_query.shape[1] // hd * rows
    two, width, chans = w_in.shape
    freq = jnp.asarray(np.exp(-math.log(ROPE_BASE) * 2.0 * np.arange(half) / (2 * half)).reshape(1, half), F32)
    operands = (
        tokens, attn_gain.reshape(1, -1), w_query, w_key, w_value, w_out,
        keys.reshape(rows, span, hd), values.reshape(rows, span, hd), lengths.reshape(1, -1), positions.reshape(1, -1),
        mamba_gain.reshape(1, -1), jnp.transpose(w_in, (0, 2, 1)).reshape(two * chans, width),
        conv_weight, conv_bias.reshape(1, -1), jnp.transpose(conv_state, (1, 0, 2)), w_xproj,
        jnp.transpose(w_dt), dt_bias.reshape(1, -1), a_log, skip_gain.reshape(1, -1), ssm, w_mout, freq,
    )
    pad = -(-w_xproj.shape[1] // 128) * 128
    dma = pltpu.SemaphoreType.DMA
    buffers = [
        ((nz, rows, w_query.shape[1] + 128), F32),
        ((2, rows, w_query.shape[1] + 128), F32),
        ((rows, w_query.shape[1] + 128), F32),
        ((rows, w_query.shape[1] + 128), F32),
        ((nz, rows, 2 * hd), F32),
        ((rows, hd), F32),
        ((rows, hd), F32),
        ((nz, qrows, hd), BF16),
        ((nz, 1, 128), F32),
        ((nx, rows, feats), BF16),
        ((nz, rows, feats), BF16),
        ((nx, rows, pad), BF16),
        ((nz, rows, pad), BF16),
        ((nz, rows, feats), BF16),
        ((nz, rows, feats), BF16),
        ((nx, rows, feats), F32),
    ]
    flag = pltpu.SemaphoreType.REGULAR
    sems = [dma((nz,)), dma((nz,)), dma((2,)), dma((2,)), flag((3,)), flag, flag] + [dma] * 8 + [dma, dma((3,))] + [dma] * 8
    hidden, state = pl.pallas_call(
        functools.partial(kernel, nz, nx),
        out_shape=(
            pltpu.VMEM((rows, feats), BF16),
            pltpu.VMEM(ssm.shape, F32),
        ),
        in_specs=[pl.BlockSpec(memory_space=pltpu.HBM)] * len(operands),
        out_specs=(pl.BlockSpec(memory_space=pltpu.VMEM), pl.BlockSpec(memory_space=pltpu.VMEM)),
        scratch_shapes=[pltpu.VMEM(o.shape, o.dtype) for o in operands]
        + [dma((len(operands),))]
        + [pltpu.VMEM(shape, kind) for shape, kind in buffers]
        + sems,
        compiler_params=pltpu.CompilerParams(
            collective_id=0, has_side_effects=True, vmem_limit_bytes=48 * 2**20
        ),
        name="decode_step",
    )(*[pltpu.with_memory_space_constraint(o, pltpu.HBM) for o in operands])
    return pl.pallas_call(
        put_out,
        out_shape=(jax.ShapeDtypeStruct((rows, feats), BF16), jax.ShapeDtypeStruct(ssm.shape, F32)),
        in_specs=[pl.BlockSpec(memory_space=pltpu.VMEM)] * 2,
        out_specs=(pl.BlockSpec(memory_space=pltpu.HBM), pl.BlockSpec(memory_space=pltpu.HBM)),
        scratch_shapes=[dma((2,))],
        name="put_out",
        compiler_params=pltpu.CompilerParams(vmem_limit_bytes=2**20),
    )(*[pltpu.with_memory_space_constraint(o, pltpu.VMEM) for o in (hidden, state)])


def solution(mesh):
    batch = ("rep", "sub")
    chan = ("seq", "head")
    in_specs = (
        P(batch, "seq"), P("seq"), P("seq", "head"), P("seq", "head"), P("seq", "head"), P("head", "seq"),
        P(batch, "head", "seq", None), P(batch, "head", "seq", None), P(batch), P(batch), P(), P(None, None, chan),
        P(None, chan), P(chan), P(batch, None, chan), P(chan, None), P(None, chan), P(chan), P(None, chan), P(chan),
        P(batch, None, chan), P(chan, None),
    )
    out_specs = (P(batch, "seq"), P(batch, None, chan))
    body = functools.partial(local, mesh.shape["seq"], mesh.shape["head"])
    return jax.shard_map(body, mesh=mesh, in_specs=in_specs, out_specs=out_specs, check_vma=False)
```

```python
import functools
import math

import jax
import jax.numpy as jnp
import numpy as np
from jax import lax
from jax.experimental import pallas as pl
from jax.experimental.pallas import tpu as pltpu
from jax.sharding import PartitionSpec as P

NORM_EPS = 1e-05
FLOOR = -1e30
ROPE_BASE = 10000.0
MESH = pl.DeviceIdType.MESH
F32 = jnp.float32
BF16 = jnp.bfloat16


def far_first(n):
    return sorted(range(1, n), key=lambda k: -min(k, n - k))


def near_first(n):
    return far_first(n)[::-1]


def dot(a, b):
    return lax.dot_general(a, b, (((1,), (0,)), ((), ())), preferred_element_type=F32)


def dot_t(a, b):
    return lax.dot_general(a, b, (((1,), (1,)), ((), ())), preferred_element_type=F32)


def diagonal(shape):
    return lax.broadcasted_iota(jnp.int32, shape, 0) == lax.broadcasted_iota(jnp.int32, shape, 1)


def column_to_row(column):
    rows = column.shape[0]
    spread = jnp.where(diagonal((rows, 128)), jnp.broadcast_to(column, (rows, 128)), 0.0)
    return jnp.sum(spread, axis=0, keepdims=True)


def row_to_column(row, rows):
    spread = jnp.where(diagonal((rows, row.shape[1])), jnp.broadcast_to(row, (rows, row.shape[1])), 0.0)
    return jnp.sum(spread, axis=1, keepdims=True)


def send_all(axis, n, buffer, send_sem, recv_sem):
    me = lax.axis_index(axis)
    for k in far_first(n):
        pltpu.make_async_remote_copy(
            src_ref=buffer.at[0],
            dst_ref=buffer.at[k],
            send_sem=send_sem,
            recv_sem=recv_sem(k) if callable(recv_sem) else recv_sem,
            device_id={axis: lax.rem(me + k, n)},
            device_id_type=MESH,
        ).start()


def wait_for(buffer, sem, slots):
    part = buffer.at[pl.ds(0, slots)]
    pltpu.make_async_copy(part, part, sem).wait()


def kernel(nz, nx, *refs):
    (
        tokens_h, attn_gain_h, w_query_h, w_key_h, w_value_h, w_out_h, keys_h, values_h, lengths_h, positions_h,
        mamba_gain_h, w_in_h, conv_weight_h, conv_bias_h, conv_state_h, w_xproj_h, w_dt_h, dt_bias_h, a_log_h,
        skip_gain_h, ssm_h, w_mout_h, freq_h,
        hidden_o, state_o,
        tokens, attn_gain, w_query, w_key, w_value, w_out, keys, values, lengths, positions,
        mamba_gain, w_in, conv_weight, conv_bias, conv_state, w_xproj, w_dt, dt_bias, a_log,
        skip_gain, ssm, w_mout, freq,
        load_sem,
        q_buf, below, up_to, total_q, kv_buf, knew, vnew, acc_buf, aux_buf, part_buf, mid_buf, px_buf, pz_buf,
        out_src, share_buf, fin_buf,
        s_q, r_q, s_up, r_up, go, ready_x, ready, s_kv, r_kv, s_acc, r_acc, s_aux, r_aux, s_part, r_part, s_mid, r_mid,
        s_px, r_px, s_pz, r_pz, s_sh, r_sh, s_fin, r_fin,
    ) = refs
    z = lax.axis_index("seq")
    x = lax.axis_index("head")
    place = lax.rem(z + nz - 1, nz)
    up = lax.rem(z + 1, nz)
    is_owner = place == 0

    loads = {}
    pairs = dict(
        tokens=(tokens_h, tokens), attn_gain=(attn_gain_h, attn_gain), w_query=(w_query_h, w_query), w_key=(w_key_h, w_key),
        w_value=(w_value_h, w_value), positions=(positions_h, positions), freq=(freq_h, freq), lengths=(lengths_h, lengths),
        keys=(keys_h, keys), values=(values_h, values), w_out=(w_out_h, w_out), mamba_gain=(mamba_gain_h, mamba_gain),
        w_in=(w_in_h, w_in), conv_weight=(conv_weight_h, conv_weight), conv_bias=(conv_bias_h, conv_bias),
        conv_state=(conv_state_h, conv_state), w_xproj=(w_xproj_h, w_xproj), w_dt=(w_dt_h, w_dt), dt_bias=(dt_bias_h, dt_bias),
        a_log=(a_log_h, a_log), skip_gain=(skip_gain_h, skip_gain), ssm=(ssm_h, ssm), w_mout=(w_mout_h, w_mout),
    )
    quarter = w_query.shape[0] // 4
    del pairs["w_query"]
    for i in range(4):
        part = pl.ds(i * quarter, quarter)
        loads["w_query", i] = pltpu.make_async_copy(w_query_h.at[part], w_query.at[part], load_sem.at[len(pairs) + i])
        loads["w_query", i].start()
    for i, (name, (source, target)) in enumerate(pairs.items()):
        loads[name] = pltpu.make_async_copy(source, target, load_sem.at[i])
        loads[name].start()

    def need(*names):
        for name in names:
            loads.pop(name).wait()

    barrier = pltpu.get_barrier_semaphore()

    @pl.when(place == 0)
    def _():
        for k in far_first(nx):
            pl.semaphore_signal(barrier, inc=1, device_id={"head": lax.rem(x + k, nx)}, device_id_type=MESH)

    pl.semaphore_wait(barrier, jnp.where(place == 0, nx - 1, 1))

    @pl.when(place < nz - 1)
    def _():
        pl.semaphore_signal(barrier, inc=1, device_id={"seq": up}, device_id_type=MESH)

    for i in (1, 2):

        @pl.when(place >= i)
        def _(i=i):
            pl.semaphore_signal(go.at[i], inc=1, device_id={"seq": lax.rem(z + nz - i, nz)}, device_id_type=MESH)

    rows = tokens.shape[0]
    feats = tokens.shape[1]
    hd = keys.shape[2]
    span = keys.shape[1]
    groups = w_query.shape[1] // hd
    qrows = groups * rows
    width = feats * nz
    chans = w_xproj.shape[0]
    rank = w_dt.shape[1]
    nstate = a_log.shape[0]

    need("tokens", "attn_gain", *[("w_query", i) for i in range(4)])
    token_f = tokens[...].astype(F32)
    lifted = (token_f * attn_gain[...]).astype(BF16)
    qw = w_query.shape[1]
    part = dot(lifted, w_query[...])
    q_buf[0, :, :qw] = part.astype(BF16)
    left = jnp.sum(token_f * token_f, axis=1, keepdims=True)
    lane = lax.broadcasted_iota(jnp.int32, (rows, 128), 1)
    up_to[:, :qw] = part
    up_to[:, qw:] = jnp.where(lane == 0, left, 0.0)
    terms = jnp.zeros((rows, 128), F32)
    for i in range(3):
        term = left.astype(BF16).astype(F32)
        terms = jnp.where(lane == i, term, terms)
        left = left - term
    q_buf[0, :, qw:] = terms.astype(BF16)

    for k in far_first(nz):

        @pl.when(place >= k)
        def _(k=k):
            pltpu.make_async_remote_copy(
                src_ref=q_buf.at[0], dst_ref=q_buf.at[k], send_sem=s_q.at[k], recv_sem=r_q.at[k],
                device_id={"seq": lax.rem(z + nz - k, nz)}, device_id_type=MESH,
            ).start()

    need("w_key", "w_value")
    kv_buf[0, :, :hd] = dot(lifted, w_key[...])
    kv_buf[0, :, hd:] = dot(lifted, w_value[...])

    @pl.when(place > 0)
    def _():
        pltpu.make_async_remote_copy(
            src_ref=kv_buf.at[0], dst_ref=kv_buf.at[place], send_sem=s_kv, recv_sem=r_kv,
            device_id={"seq": 1}, device_id_type=MESH,
        ).start()

    knew[...] = jnp.zeros_like(knew)
    vnew[...] = jnp.zeros_like(vnew)
    need("positions", "freq", "lengths")
    angle = row_to_column(positions[...].astype(F32), rows) * freq[...]
    cosine = jnp.cos(angle)
    sine = jnp.sin(angle)
    cosine = jnp.concatenate([cosine, cosine], axis=1)
    sine = jnp.concatenate([-sine, sine], axis=1)

    def rotated(v):
        return v * cosine + pltpu.roll(v, hd // 2, 1) * sine

    limit = row_to_column(lengths[...].astype(F32), rows)
    limit = jnp.concatenate([limit] * groups, axis=0)
    spot = (lax.broadcasted_iota(jnp.int32, (qrows, span), 1) + z * span).astype(F32)
    live = spot < limit
    row_of = lax.broadcasted_iota(jnp.int32, (qrows, hd), 0) % rows
    row_of_wide = lax.broadcasted_iota(jnp.int32, (qrows, span), 0) % rows

    @pl.when(place >= 2)
    def _():
        pltpu.make_async_copy(below.at[1], below.at[1], r_up.at[1]).wait()
        up_to[...] += below[1]

    total_q[...] = up_to[...]

    for i in (1, 2):

        @pl.when(place < nz - i)
        def _(i=i):
            pl.semaphore_wait(go.at[i], 1)
            pltpu.make_async_remote_copy(
                src_ref=up_to, dst_ref=below.at[i - 1], send_sem=s_up.at[i - 1], recv_sem=r_up.at[i - 1],
                device_id={"seq": lax.rem(z + i, nz)}, device_id_type=MESH,
            ).start()

    @pl.when(place >= 1)
    def _():
        pltpu.make_async_copy(below.at[0], below.at[0], r_up.at[0]).wait()
        total_q[...] += below[0]

    for k in range(1, nz):

        @pl.when(place + k < nz)
        def _(k=k):
            pltpu.make_async_copy(q_buf.at[k], q_buf.at[k], r_q.at[k]).wait()
            total_q[...] += q_buf[k].astype(F32)

    @pl.when(place == 0)
    def _():
        for k in far_first(nx):
            pl.semaphore_signal(ready_x, inc=1, device_id={"head": lax.rem(x + k, nx)}, device_id_type=MESH)

    r_a = lax.rsqrt(jnp.sum(total_q[:, qw:], axis=1, keepdims=True) / width + NORM_EPS)

    @pl.when(is_owner)
    def _():
        wait_for(kv_buf, r_kv, nz - 1)
        kv = kv_buf[0]
        for k in range(1, nz):
            kv = kv + kv_buf[k]
        knew[...] = rotated(kv[:, :hd] * r_a).astype(BF16).astype(F32)
        vnew[...] = (kv[:, hd:] * r_a).astype(BF16).astype(F32)

    q = [rotated(total_q[:, g * hd : (g + 1) * hd] * r_a) for g in range(groups)]
    q = jnp.concatenate(q, axis=0).astype(BF16)

    need("keys")
    scores = jnp.zeros((qrows, span), F32)
    for b in range(rows):
        scores = jnp.where(row_of_wide == b, dot_t(q, keys[b]), scores)
    scale = hd ** (-0.5)
    scores = scores * scale
    top = jnp.max(jnp.where(live, scores, FLOOR), axis=1, keepdims=True)
    fresh = jnp.sum(q.astype(F32) * jnp.concatenate([knew[...]] * groups, axis=0), axis=1, keepdims=True) * scale
    mine = jnp.broadcast_to(is_owner, fresh.shape)
    top = jnp.maximum(top, jnp.where(mine, fresh, FLOOR))
    weights = jnp.where(live, jnp.exp(scores - top), 0.0)
    new_weight = jnp.where(mine, jnp.exp(fresh - top), 0.0)
    total = jnp.sum(weights, axis=1, keepdims=True) + new_weight
    weights = weights.astype(BF16)
    need("values")
    acc = jnp.zeros((qrows, hd), F32)
    for b in range(rows):
        acc = jnp.where(row_of == b, dot(weights, values[b]), acc)
    acc = acc + new_weight * jnp.concatenate([vnew[...]] * groups, axis=0)
    acc_buf[0] = acc.astype(BF16)
    aux_buf[0] = column_to_row(top) + pltpu.roll(column_to_row(total), 64, 1)
    send_all("seq", nz, aux_buf, s_aux, r_aux)
    send_all("seq", nz, acc_buf, s_acc, r_acc)

    @pl.when(place == 0)
    def _():
        pl.semaphore_wait(ready_x, nx - 1)
        for k in far_first(nz):
            pl.semaphore_signal(ready, inc=1, device_id={"seq": lax.rem(z + k, nz)}, device_id_type=MESH)


    need("w_out")
    wait_for(aux_buf, r_aux, nz - 1)
    aux = jnp.concatenate([aux_buf[k] for k in range(nz)], axis=0)
    factor = jnp.exp(aux - jnp.max(aux, axis=0, keepdims=True))
    whole = jnp.sum(factor * pltpu.roll(aux, 64, 1), axis=0, keepdims=True)
    lane = lax.broadcasted_iota(jnp.int32, (nz, 128), 1)
    share = jnp.where(lane < qrows, factor / whole, 0.0)
    share = jnp.concatenate([share, jnp.zeros((128 - nz, 128), F32)], axis=0).T
    wait_for(acc_buf, r_acc, nz - 1)
    attended = share[:qrows, 0:1] * acc_buf[0].astype(F32)
    for k in range(1, nz):
        attended = attended + share[:qrows, k : k + 1] * acc_buf[k].astype(F32)
    attended = jnp.concatenate([attended[g * rows : (g + 1) * rows] for g in range(groups)], axis=1).astype(BF16)
    part_buf[0] = dot(attended, w_out[...]).astype(BF16)

    @pl.when(place > 0)
    def _():
        pl.semaphore_wait(ready, 1)

    send_all("head", nx, part_buf, s_part, r_part)
    need("mamba_gain", "w_in")
    wait_for(part_buf, r_part, nx - 1)
    summed = part_buf[lax.rem(x, nx)].astype(F32)
    for j in range(1, nx):
        summed = summed + part_buf[lax.rem(x - j + nx, nx)].astype(F32)
    mid = (token_f + summed).astype(BF16)
    mid_buf[0] = mid
    circle = sorted(range(1, nz), key=lambda k: min(k, nz - k))
    ends = (0, nz // 2, max(nz // 2, nz - 4), nz - 1)
    rings = [circle[i:j] for i, j in zip(ends, ends[1:]) if j > i]
    ring_of = {k: i for i, r in enumerate(rings) for k in r}
    send_all("seq", nz, mid_buf, s_mid, lambda k: r_mid.at[ring_of[k]])

    def block_of(k):
        at = pl.multiple_of(lax.rem(z - k + nz, nz) * feats, feats)
        block = mid_buf[k].astype(F32)
        raised = (block * mamba_gain[:, pl.ds(at, feats)]).astype(BF16)
        return block * block, dot_t(raised, w_in[:, pl.ds(at, feats)])

    squares, both = block_of(0)
    for i, ring in enumerate(rings):
        wait_for(mid_buf, r_mid.at[i], len(ring))
        for k in ring:
            more, extra = block_of(k)
            squares = squares + more
            both = both + extra
    both = both * lax.rsqrt(jnp.sum(squares, axis=1, keepdims=True) / width + NORM_EPS)
    inner = both[:, :chans]
    gate = both[:, chans:]

    need("conv_weight", "conv_bias", "conv_state", "w_xproj")
    mixed = inner * conv_weight[3:4, :] + conv_bias[...]
    for k in range(3):
        mixed = mixed + conv_state[k] * conv_weight[k : k + 1, :]
    u = mixed / (1.0 + jnp.exp(-mixed))
    proj = dot(u.astype(BF16), w_xproj[...])
    px_buf[0] = jnp.concatenate([proj, jnp.zeros((rows, px_buf.shape[2] - proj.shape[1]), F32)], axis=1).astype(BF16)
    send_all("head", nx, px_buf, s_px, r_px)
    need("w_dt", "dt_bias", "a_log", "skip_gain", "ssm", "w_mout")
    decay_rate = -jnp.exp(a_log[...])
    gated = gate / (1.0 + jnp.exp(-gate))
    wait_for(px_buf, r_px, nx - 1)
    proj = px_buf[0].astype(F32)
    for k in range(1, nx):
        proj = proj + px_buf[k].astype(F32)
    pz_buf[0] = proj.astype(BF16)
    send_all("seq", nz, pz_buf, s_pz, r_pz)
    wait_for(pz_buf, r_pz, nz - 1)
    proj = pz_buf[0].astype(F32)
    for k in range(1, nz):
        proj = proj + pz_buf[k].astype(F32)

    pre = dot_t(proj[:, :rank].astype(BF16), w_dt[...]) + dt_bias[...]
    step = jnp.maximum(pre, 0.0) + jnp.log(1.0 + jnp.exp(-jnp.abs(pre)))
    maps = jnp.concatenate([proj[:, rank : rank + 128], jnp.zeros((128 - rows, 128), F32)], axis=0).T
    drive = step * u
    reads = []
    for b in range(rows):
        state = (
            jnp.exp(step[b : b + 1, :] * decay_rate) * ssm[b]
            + drive[b : b + 1, :] * maps[:nstate, b : b + 1]
        )
        state_o[b] = state
        reads.append(jnp.sum(maps[nstate : 2 * nstate, b : b + 1] * state, axis=0, keepdims=True))
    y = (jnp.concatenate(reads, axis=0) + skip_gain[...] * u) * gated
    y = y.astype(BF16)

    def out_block(k):
        at = pl.multiple_of(lax.rem(z + k, nz) * feats, feats)
        return dot(y, w_mout[:, pl.ds(at, feats)]).astype(BF16)

    for k in far_first(nz):
        out_src[k] = out_block(k)
        pltpu.make_async_remote_copy(
            src_ref=out_src.at[k], dst_ref=share_buf.at[k], send_sem=s_sh, recv_sem=r_sh,
            device_id={"seq": lax.rem(z + k, nz)}, device_id_type=MESH,
        ).start()
    result = out_block(0).astype(F32)
    wait_for(share_buf, r_sh, nz - 1)
    for k in range(1, nz):
        result = result + share_buf[k].astype(F32)
    fin_buf[0] = result
    send_all("head", nx, fin_buf, s_fin, r_fin)

    for k in range(1, nz):

        @pl.when(place >= k)
        def _(k=k):
            pltpu.make_async_copy(q_buf.at[0], q_buf.at[0], s_q.at[k]).wait()

    @pl.when(place > 0)
    def _():
        pltpu.make_async_copy(kv_buf.at[0], kv_buf.at[0], s_kv).wait()

    for i in (1, 2):

        @pl.when(place < nz - i)
        def _(i=i):
            pltpu.make_async_copy(up_to, up_to, s_up.at[i - 1]).wait()

    wait_for(aux_buf, s_aux, nz - 1)
    wait_for(acc_buf, s_acc, nz - 1)
    wait_for(part_buf, s_part, nx - 1)
    wait_for(mid_buf, s_mid, nz - 1)
    wait_for(px_buf, s_px, nx - 1)
    wait_for(pz_buf, s_pz, nz - 1)
    wait_for(share_buf, s_sh, nz - 1)
    wait_for(fin_buf, r_fin, nx - 1)
    result = fin_buf[lax.rem(x, nx)]
    for j in range(1, nx):
        result = result + fin_buf[lax.rem(x - j + nx, nx)]
    hidden_o[...] = (mid.astype(F32) + result).astype(BF16)
    wait_for(fin_buf, s_fin, nx - 1)


def put_out(hidden, state, hidden_o, state_o, sem):
    copies = [pltpu.make_async_copy(hidden, hidden_o, sem.at[0]), pltpu.make_async_copy(state, state_o, sem.at[1])]
    for copy in copies:
        copy.start()
    for copy in copies:
        copy.wait()


def local(nz, nx, *args):
    (
        tokens, attn_gain, w_query, w_key, w_value, w_out, keys, values, lengths, positions, mamba_gain, w_in,
        conv_weight, conv_bias, conv_state, w_xproj, w_dt, dt_bias, a_log, skip_gain, ssm, w_mout,
    ) = args
    rows, feats = tokens.shape
    hd = keys.shape[3]
    span = keys.shape[2]
    half = hd // 2
    qrows = w_query.shape[1] // hd * rows
    two, width, chans = w_in.shape
    freq = jnp.asarray(np.exp(-math.log(ROPE_BASE) * 2.0 * np.arange(half) / (2 * half)).reshape(1, half), F32)
    operands = (
        tokens, attn_gain.reshape(1, -1), w_query, w_key, w_value, w_out,
        keys.reshape(rows, span, hd), values.reshape(rows, span, hd), lengths.reshape(1, -1), positions.reshape(1, -1),
        mamba_gain.reshape(1, -1), jnp.transpose(w_in, (0, 2, 1)).reshape(two * chans, width),
        conv_weight, conv_bias.reshape(1, -1), jnp.transpose(conv_state, (1, 0, 2)), w_xproj,
        jnp.transpose(w_dt), dt_bias.reshape(1, -1), a_log, skip_gain.reshape(1, -1), ssm, w_mout, freq,
    )
    pad = -(-w_xproj.shape[1] // 128) * 128
    dma = pltpu.SemaphoreType.DMA
    buffers = [
        ((nz, rows, w_query.shape[1] + 128), BF16),
        ((2, rows, w_query.shape[1] + 128), F32),
        ((rows, w_query.shape[1] + 128), F32),
        ((rows, w_query.shape[1] + 128), F32),
        ((nz, rows, 2 * hd), F32),
        ((rows, hd), F32),
        ((rows, hd), F32),
        ((nz, qrows, hd), BF16),
        ((nz, 1, 128), F32),
        ((nx, rows, feats), BF16),
        ((nz, rows, feats), BF16),
        ((nx, rows, pad), BF16),
        ((nz, rows, pad), BF16),
        ((nz, rows, feats), BF16),
        ((nz, rows, feats), BF16),
        ((nx, rows, feats), F32),
    ]
    flag = pltpu.SemaphoreType.REGULAR
    sems = [dma((nz,)), dma((nz,)), dma((2,)), dma((2,)), flag((3,)), flag, flag] + [dma] * 8 + [dma, dma((3,))] + [dma] * 8
    hidden, state = pl.pallas_call(
        functools.partial(kernel, nz, nx),
        out_shape=(
            pltpu.VMEM((rows, feats), BF16),
            pltpu.VMEM(ssm.shape, F32),
        ),
        in_specs=[pl.BlockSpec(memory_space=pltpu.HBM)] * len(operands),
        out_specs=(pl.BlockSpec(memory_space=pltpu.VMEM), pl.BlockSpec(memory_space=pltpu.VMEM)),
        scratch_shapes=[pltpu.VMEM(o.shape, o.dtype) for o in operands]
        + [dma((len(operands) + 3,))]
        + [pltpu.VMEM(shape, kind) for shape, kind in buffers]
        + sems,
        compiler_params=pltpu.CompilerParams(
            collective_id=0, has_side_effects=True, vmem_limit_bytes=48 * 2**20
        ),
        name="decode_step",
    )(*[pltpu.with_memory_space_constraint(o, pltpu.HBM) for o in operands])
    return pl.pallas_call(
        put_out,
        out_shape=(jax.ShapeDtypeStruct((rows, feats), BF16), jax.ShapeDtypeStruct(ssm.shape, F32)),
        in_specs=[pl.BlockSpec(memory_space=pltpu.VMEM)] * 2,
        out_specs=(pl.BlockSpec(memory_space=pltpu.HBM), pl.BlockSpec(memory_space=pltpu.HBM)),
        scratch_shapes=[dma((2,))],
        name="put_out",
        compiler_params=pltpu.CompilerParams(vmem_limit_bytes=2**20),
    )(*[pltpu.with_memory_space_constraint(o, pltpu.VMEM) for o in (hidden, state)])


def solution(mesh):
    batch = ("rep", "sub")
    chan = ("seq", "head")
    in_specs = (
        P(batch, "seq"), P("seq"), P("seq", "head"), P("seq", "head"), P("seq", "head"), P("head", "seq"),
        P(batch, "head", "seq", None), P(batch, "head", "seq", None), P(batch), P(batch), P(), P(None, None, chan),
        P(None, chan), P(chan), P(batch, None, chan), P(chan, None), P(None, chan), P(chan), P(None, chan), P(chan),
        P(batch, None, chan), P(chan, None),
    )
    out_specs = (P(batch, "seq"), P(batch, None, chan))
    body = functools.partial(local, mesh.shape["seq"], mesh.shape["head"])
    return jax.shard_map(body, mesh=mesh, in_specs=in_specs, out_specs=out_specs, check_vma=False)
```

```python
import functools
import math

import jax
import jax.numpy as jnp
import numpy as np
from jax import lax
from jax.experimental import pallas as pl
from jax.experimental.pallas import tpu as pltpu
from jax.sharding import PartitionSpec as P

NORM_EPS = 1e-05
FLOOR = -1e30
ROPE_BASE = 10000.0
MESH = pl.DeviceIdType.MESH
F32 = jnp.float32
BF16 = jnp.bfloat16


def far_first(n):
    return sorted(range(1, n), key=lambda k: -min(k, n - k))


def near_first(n):
    return far_first(n)[::-1]


def dot(a, b):
    return lax.dot_general(a, b, (((1,), (0,)), ((), ())), preferred_element_type=F32)


def dot_t(a, b):
    return lax.dot_general(a, b, (((1,), (1,)), ((), ())), preferred_element_type=F32)


def diagonal(shape):
    return lax.broadcasted_iota(jnp.int32, shape, 0) == lax.broadcasted_iota(jnp.int32, shape, 1)


def column_to_row(column):
    rows = column.shape[0]
    spread = jnp.where(diagonal((rows, 128)), jnp.broadcast_to(column, (rows, 128)), 0.0)
    return jnp.sum(spread, axis=0, keepdims=True)


def row_to_column(row, rows):
    spread = jnp.where(diagonal((rows, row.shape[1])), jnp.broadcast_to(row, (rows, row.shape[1])), 0.0)
    return jnp.sum(spread, axis=1, keepdims=True)


def in_terms(row, count):
    lane = lax.broadcasted_iota(jnp.int32, row.shape, 1)
    left = jnp.where(lane < count, row, 0.0)
    terms = jnp.zeros_like(row)
    for i in range(3):
        term = left.astype(BF16).astype(F32)
        terms = terms + (pltpu.roll(term, i * count, 1) if i else term)
        left = left - term
    return terms


def of_terms(terms, count):
    return terms + pltpu.roll(terms, 128 - count, 1) + pltpu.roll(terms, 128 - 2 * count, 1)


def send_all(axis, n, buffer, send_sem, recv_sem):
    me = lax.axis_index(axis)
    for k in far_first(n):
        pltpu.make_async_remote_copy(
            src_ref=buffer.at[0],
            dst_ref=buffer.at[k],
            send_sem=send_sem,
            recv_sem=recv_sem(k) if callable(recv_sem) else recv_sem,
            device_id={axis: lax.rem(me + k, n)},
            device_id_type=MESH,
        ).start()


def wait_for(buffer, sem, slots):
    part = buffer.at[pl.ds(0, slots)]
    pltpu.make_async_copy(part, part, sem).wait()


def kernel(nz, nx, *refs):
    (
        tokens_h, attn_gain_h, w_query_h, w_key_h, w_value_h, w_out_h, keys_h, values_h, lengths_h, positions_h,
        mamba_gain_h, w_in_h, conv_weight_h, conv_bias_h, conv_state_h, w_xproj_h, w_dt_h, dt_bias_h, a_log_h,
        skip_gain_h, ssm_h, w_mout_h, freq_h,
        hidden_o, state_o,
        tokens, attn_gain, w_query, w_key, w_value, w_out, keys, values, lengths, positions,
        mamba_gain, w_in, conv_weight, conv_bias, conv_state, w_xproj, w_dt, dt_bias, a_log,
        skip_gain, ssm, w_mout, freq,
        load_sem,
        q_buf, below, up_to, total_q, kv_buf, knew, vnew, acc_buf, part_buf, mid_buf, px_buf, pz_buf,
        out_src, share_buf, fin_buf,
        s_q, r_q, s_up, r_up, go, ready_x, ready, s_kv, r_kv, s_acc, r_acc, s_part, r_part, s_mid, r_mid,
        s_px, r_px, s_pz, r_pz, s_sh, r_sh, s_fin, r_fin,
    ) = refs
    z = lax.axis_index("seq")
    x = lax.axis_index("head")
    first = jnp.where(x == 0, 1, 0)
    place = lax.rem(z + nz - first, nz)
    up = lax.rem(z + 1, nz)
    is_owner = place == 0

    loads = {}
    pairs = dict(
        tokens=(tokens_h, tokens), attn_gain=(attn_gain_h, attn_gain), w_query=(w_query_h, w_query), w_key=(w_key_h, w_key),
        w_value=(w_value_h, w_value), positions=(positions_h, positions), freq=(freq_h, freq), lengths=(lengths_h, lengths),
        keys=(keys_h, keys), values=(values_h, values), w_out=(w_out_h, w_out), mamba_gain=(mamba_gain_h, mamba_gain),
        w_in=(w_in_h, w_in), conv_weight=(conv_weight_h, conv_weight), conv_bias=(conv_bias_h, conv_bias),
        conv_state=(conv_state_h, conv_state), w_xproj=(w_xproj_h, w_xproj), w_dt=(w_dt_h, w_dt), dt_bias=(dt_bias_h, dt_bias),
        a_log=(a_log_h, a_log), skip_gain=(skip_gain_h, skip_gain), ssm=(ssm_h, ssm), w_mout=(w_mout_h, w_mout),
    )
    quarter = w_query.shape[0] // 4
    del pairs["w_query"]
    for i in range(4):
        part = pl.ds(i * quarter, quarter)
        loads["w_query", i] = pltpu.make_async_copy(w_query_h.at[part], w_query.at[part], load_sem.at[len(pairs) + i])
        loads["w_query", i].start()
    for i, (name, (source, target)) in enumerate(pairs.items()):
        loads[name] = pltpu.make_async_copy(source, target, load_sem.at[i])
        loads[name].start()

    def need(*names):
        for name in names:
            loads.pop(name).wait()

    barrier = pltpu.get_barrier_semaphore()

    def hub(k):
        peer = lax.rem(x + k, nx)
        return {"head": peer, "seq": jnp.where(peer == 0, 1, 0)}


    @pl.when(place == 0)
    def _():
        for k in far_first(nx):
            pl.semaphore_signal(barrier, inc=1, device_id=hub(k), device_id_type=MESH)

    pl.semaphore_wait(barrier, jnp.where(place == 0, nx - 1, 1))

    @pl.when(place < nz - 1)
    def _():
        pl.semaphore_signal(barrier, inc=1, device_id={"seq": up}, device_id_type=MESH)

    for i in (1, 2):

        @pl.when(place >= i)
        def _(i=i):
            pl.semaphore_signal(go.at[i], inc=1, device_id={"seq": lax.rem(z + nz - i, nz)}, device_id_type=MESH)

    rows = tokens.shape[0]
    feats = tokens.shape[1]
    hd = keys.shape[2]
    span = keys.shape[1]
    groups = w_query.shape[1] // hd
    qrows = groups * rows
    width = feats * nz
    chans = w_xproj.shape[0]
    rank = w_dt.shape[1]
    nstate = a_log.shape[0]

    need("tokens", "attn_gain", *[("w_query", i) for i in range(4)])
    token_f = tokens[...].astype(F32)
    lifted = (token_f * attn_gain[...]).astype(BF16)
    qw = w_query.shape[1]
    part = dot(lifted, w_query[...])
    q_buf[0, :, :qw] = part.astype(BF16)
    left = jnp.sum(token_f * token_f, axis=1, keepdims=True)
    lane = lax.broadcasted_iota(jnp.int32, (rows, 128), 1)
    up_to[:, :qw] = part
    up_to[:, qw:] = jnp.where(lane == 0, left, 0.0)
    terms = jnp.zeros((rows, 128), F32)
    for i in range(3):
        term = left.astype(BF16).astype(F32)
        terms = jnp.where(lane == i, term, terms)
        left = left - term
    q_buf[0, :, qw:] = terms.astype(BF16)

    for k in far_first(nz):

        @pl.when(place >= k)
        def _(k=k):
            pltpu.make_async_remote_copy(
                src_ref=q_buf.at[0], dst_ref=q_buf.at[k], send_sem=s_q.at[k], recv_sem=r_q.at[k],
                device_id={"seq": lax.rem(z + nz - k, nz)}, device_id_type=MESH,
            ).start()

    need("w_key", "w_value")
    kv_buf[0, :, :hd] = dot(lifted, w_key[...])
    kv_buf[0, :, hd:] = dot(lifted, w_value[...])

    @pl.when(place > 0)
    def _():
        pltpu.make_async_remote_copy(
            src_ref=kv_buf.at[0], dst_ref=kv_buf.at[place], send_sem=s_kv, recv_sem=r_kv,
            device_id={"seq": first}, device_id_type=MESH,
        ).start()

    knew[...] = jnp.zeros_like(knew)
    vnew[...] = jnp.zeros_like(vnew)
    need("positions", "freq", "lengths")
    angle = row_to_column(positions[...].astype(F32), rows) * freq[...]
    cosine = jnp.cos(angle)
    sine = jnp.sin(angle)
    cosine = jnp.concatenate([cosine, cosine], axis=1)
    sine = jnp.concatenate([-sine, sine], axis=1)

    def rotated(v):
        return v * cosine + pltpu.roll(v, hd // 2, 1) * sine

    limit = row_to_column(lengths[...].astype(F32), rows)
    limit = jnp.concatenate([limit] * groups, axis=0)
    spot = (lax.broadcasted_iota(jnp.int32, (qrows, span), 1) + z * span).astype(F32)
    live = spot < limit
    row_of = lax.broadcasted_iota(jnp.int32, (qrows, hd), 0) % rows
    row_of_wide = lax.broadcasted_iota(jnp.int32, (qrows, span), 0) % rows

    @pl.when(place >= 2)
    def _():
        pltpu.make_async_copy(below.at[1], below.at[1], r_up.at[1]).wait()
        up_to[...] += below[1]

    total_q[...] = up_to[...]

    for i in (1, 2):

        @pl.when(place < nz - i)
        def _(i=i):
            pl.semaphore_wait(go.at[i], 1)
            pltpu.make_async_remote_copy(
                src_ref=up_to, dst_ref=below.at[i - 1], send_sem=s_up.at[i - 1], recv_sem=r_up.at[i - 1],
                device_id={"seq": lax.rem(z + i, nz)}, device_id_type=MESH,
            ).start()

    @pl.when(place >= 1)
    def _():
        pltpu.make_async_copy(below.at[0], below.at[0], r_up.at[0]).wait()
        total_q[...] += below[0]

    for k in range(1, nz):

        @pl.when(place + k < nz)
        def _(k=k):
            pltpu.make_async_copy(q_buf.at[k], q_buf.at[k], r_q.at[k]).wait()
            total_q[...] += q_buf[k].astype(F32)

    @pl.when(place == 0)
    def _():
        for k in far_first(nx):
            pl.semaphore_signal(ready_x, inc=1, device_id=hub(k), device_id_type=MESH)

    r_a = lax.rsqrt(jnp.sum(total_q[:, qw:], axis=1, keepdims=True) / width + NORM_EPS)

    @pl.when(is_owner)
    def _():
        wait_for(kv_buf, r_kv, nz - 1)
        kv = kv_buf[0]
        for k in range(1, nz):
            kv = kv + kv_buf[k]
        knew[...] = rotated(kv[:, :hd] * r_a).astype(BF16).astype(F32)
        vnew[...] = (kv[:, hd:] * r_a).astype(BF16).astype(F32)

    q = [rotated(total_q[:, g * hd : (g + 1) * hd] * r_a) for g in range(groups)]
    q = jnp.concatenate(q, axis=0).astype(BF16)

    need("keys")
    scores = jnp.zeros((qrows, span), F32)
    for b in range(rows):
        scores = jnp.where(row_of_wide == b, dot_t(q, keys[b]), scores)
    scale = hd ** (-0.5)
    scores = scores * scale
    top = jnp.max(jnp.where(live, scores, FLOOR), axis=1, keepdims=True)
    fresh = jnp.sum(q.astype(F32) * jnp.concatenate([knew[...]] * groups, axis=0), axis=1, keepdims=True) * scale
    mine = jnp.broadcast_to(is_owner, fresh.shape)
    top = jnp.maximum(top, jnp.where(mine, fresh, FLOOR))
    weights = jnp.where(live, jnp.exp(scores - top), 0.0)
    new_weight = jnp.where(mine, jnp.exp(fresh - top), 0.0)
    total = jnp.sum(weights, axis=1, keepdims=True) + new_weight
    weights = weights.astype(BF16)
    need("values")
    acc = jnp.zeros((qrows, hd), F32)
    for b in range(rows):
        acc = jnp.where(row_of == b, dot(weights, values[b]), acc)
    acc = acc + new_weight * jnp.concatenate([vnew[...]] * groups, axis=0)
    acc_buf[0, :qrows] = acc.astype(BF16)
    acc_buf[0, qrows:] = jnp.concatenate([in_terms(column_to_row(top), qrows), in_terms(column_to_row(total), qrows)]).astype(BF16)
    send_all("seq", nz, acc_buf, s_acc, r_acc)

    @pl.when(place == 0)
    def _():
        pl.semaphore_wait(ready_x, nx - 1)
        for k in far_first(nz):
            pl.semaphore_signal(ready, inc=1, device_id={"seq": lax.rem(z + k, nz)}, device_id_type=MESH)


    need("w_out")
    wait_for(acc_buf, r_acc, nz - 1)
    aux = [acc_buf[k, qrows:].astype(F32) for k in range(nz)]
    tops = of_terms(jnp.concatenate([a[:1] for a in aux], axis=0), qrows)
    sums = of_terms(jnp.concatenate([a[1:] for a in aux], axis=0), qrows)
    factor = jnp.exp(tops - jnp.max(tops, axis=0, keepdims=True))
    whole = jnp.sum(factor * sums, axis=0, keepdims=True)
    lane = lax.broadcasted_iota(jnp.int32, (nz, 128), 1)
    share = jnp.where(lane < qrows, factor / whole, 0.0)
    share = jnp.concatenate([share, jnp.zeros((128 - nz, 128), F32)], axis=0).T
    attended = share[:qrows, 0:1] * acc_buf[0, :qrows].astype(F32)
    for k in range(1, nz):
        attended = attended + share[:qrows, k : k + 1] * acc_buf[k, :qrows].astype(F32)
    attended = jnp.concatenate([attended[g * rows : (g + 1) * rows] for g in range(groups)], axis=1).astype(BF16)
    part_buf[0] = dot(attended, w_out[...]).astype(BF16)

    @pl.when(place > 0)
    def _():
        pl.semaphore_wait(ready, 1)

    send_all("head", nx, part_buf, s_part, r_part)
    need("mamba_gain", "w_in")
    wait_for(part_buf, r_part, nx - 1)
    summed = part_buf[lax.rem(x, nx)].astype(F32)
    for j in range(1, nx):
        summed = summed + part_buf[lax.rem(x - j + nx, nx)].astype(F32)
    mid = (token_f + summed).astype(BF16)
    mid_buf[0] = mid
    circle = sorted(range(1, nz), key=lambda k: min(k, nz - k))
    ends = (0, nz // 2, max(nz // 2, nz - 4), nz - 1)
    rings = [circle[i:j] for i, j in zip(ends, ends[1:]) if j > i]
    ring_of = {k: i for i, r in enumerate(rings) for k in r}
    send_all("seq", nz, mid_buf, s_mid, lambda k: r_mid.at[ring_of[k]])

    def block_of(k):
        at = pl.multiple_of(lax.rem(z - k + nz, nz) * feats, feats)
        block = mid_buf[k].astype(F32)
        raised = (block * mamba_gain[:, pl.ds(at, feats)]).astype(BF16)
        return block * block, dot_t(raised, w_in[:, pl.ds(at, feats)])

    squares, both = block_of(0)
    for i, ring in enumerate(rings):
        wait_for(mid_buf, r_mid.at[i], len(ring))
        for k in ring:
            more, extra = block_of(k)
            squares = squares + more
            both = both + extra
    both = both * lax.rsqrt(jnp.sum(squares, axis=1, keepdims=True) / width + NORM_EPS)
    inner = both[:, :chans]
    gate = both[:, chans:]

    need("conv_weight", "conv_bias", "conv_state", "w_xproj")
    mixed = inner * conv_weight[3:4, :] + conv_bias[...]
    for k in range(3):
        mixed = mixed + conv_state[k] * conv_weight[k : k + 1, :]
    u = mixed / (1.0 + jnp.exp(-mixed))
    proj = dot(u.astype(BF16), w_xproj[...])
    px_buf[0] = jnp.concatenate([proj, jnp.zeros((rows, px_buf.shape[2] - proj.shape[1]), F32)], axis=1).astype(BF16)
    send_all("head", nx, px_buf, s_px, r_px)
    need("w_dt", "dt_bias", "a_log", "skip_gain", "ssm", "w_mout")
    decay_rate = -jnp.exp(a_log[...])
    gated = gate / (1.0 + jnp.exp(-gate))
    wait_for(px_buf, r_px, nx - 1)
    proj = px_buf[0].astype(F32)
    for k in range(1, nx):
        proj = proj + px_buf[k].astype(F32)
    pz_buf[0] = proj.astype(BF16)
    send_all("seq", nz, pz_buf, s_pz, r_pz)
    wait_for(pz_buf, r_pz, nz - 1)
    proj = pz_buf[0].astype(F32)
    for k in range(1, nz):
        proj = proj + pz_buf[k].astype(F32)

    pre = dot_t(proj[:, :rank].astype(BF16), w_dt[...]) + dt_bias[...]
    step = jnp.maximum(pre, 0.0) + jnp.log(1.0 + jnp.exp(-jnp.abs(pre)))
    maps = jnp.concatenate([proj[:, rank : rank + 128], jnp.zeros((128 - rows, 128), F32)], axis=0).T
    drive = step * u
    reads = []
    for b in range(rows):
        state = (
            jnp.exp(step[b : b + 1, :] * decay_rate) * ssm[b]
            + drive[b : b + 1, :] * maps[:nstate, b : b + 1]
        )
        state_o[b] = state
        reads.append(jnp.sum(maps[nstate : 2 * nstate, b : b + 1] * state, axis=0, keepdims=True))
    y = (jnp.concatenate(reads, axis=0) + skip_gain[...] * u) * gated
    y = y.astype(BF16)

    def out_block(k):
        at = pl.multiple_of(lax.rem(z + k, nz) * feats, feats)
        return dot(y, w_mout[:, pl.ds(at, feats)]).astype(BF16)

    for k in far_first(nz):
        out_src[k] = out_block(k)
        pltpu.make_async_remote_copy(
            src_ref=out_src.at[k], dst_ref=share_buf.at[k], send_sem=s_sh, recv_sem=r_sh,
            device_id={"seq": lax.rem(z + k, nz)}, device_id_type=MESH,
        ).start()
    result = out_block(0).astype(F32)
    wait_for(share_buf, r_sh, nz - 1)
    for k in range(1, nz):
        result = result + share_buf[k].astype(F32)
    fin_buf[0] = result
    send_all("head", nx, fin_buf, s_fin, r_fin)

    for k in range(1, nz):

        @pl.when(place >= k)
        def _(k=k):
            pltpu.make_async_copy(q_buf.at[0], q_buf.at[0], s_q.at[k]).wait()

    @pl.when(place > 0)
    def _():
        pltpu.make_async_copy(kv_buf.at[0], kv_buf.at[0], s_kv).wait()

    for i in (1, 2):

        @pl.when(place < nz - i)
        def _(i=i):
            pltpu.make_async_copy(up_to, up_to, s_up.at[i - 1]).wait()

    wait_for(acc_buf, s_acc, nz - 1)
    wait_for(part_buf, s_part, nx - 1)
    wait_for(mid_buf, s_mid, nz - 1)
    wait_for(px_buf, s_px, nx - 1)
    wait_for(pz_buf, s_pz, nz - 1)
    wait_for(share_buf, s_sh, nz - 1)
    wait_for(fin_buf, r_fin, nx - 1)
    result = fin_buf[lax.rem(x, nx)]
    for j in range(1, nx):
        result = result + fin_buf[lax.rem(x - j + nx, nx)]
    hidden_o[...] = (mid.astype(F32) + result).astype(BF16)
    wait_for(fin_buf, s_fin, nx - 1)


def put_out(hidden, state, hidden_o, state_o, sem):
    copies = [pltpu.make_async_copy(hidden, hidden_o, sem.at[0]), pltpu.make_async_copy(state, state_o, sem.at[1])]
    for copy in copies:
        copy.start()
    for copy in copies:
        copy.wait()


def local(nz, nx, *args):
    (
        tokens, attn_gain, w_query, w_key, w_value, w_out, keys, values, lengths, positions, mamba_gain, w_in,
        conv_weight, conv_bias, conv_state, w_xproj, w_dt, dt_bias, a_log, skip_gain, ssm, w_mout,
    ) = args
    rows, feats = tokens.shape
    hd = keys.shape[3]
    span = keys.shape[2]
    half = hd // 2
    qrows = w_query.shape[1] // hd * rows
    two, width, chans = w_in.shape
    freq = jnp.asarray(np.exp(-math.log(ROPE_BASE) * 2.0 * np.arange(half) / (2 * half)).reshape(1, half), F32)
    operands = (
        tokens, attn_gain.reshape(1, -1), w_query, w_key, w_value, w_out,
        keys.reshape(rows, span, hd), values.reshape(rows, span, hd), lengths.reshape(1, -1), positions.reshape(1, -1),
        mamba_gain.reshape(1, -1), jnp.transpose(w_in, (0, 2, 1)).reshape(two * chans, width),
        conv_weight, conv_bias.reshape(1, -1), jnp.transpose(conv_state, (1, 0, 2)), w_xproj,
        jnp.transpose(w_dt), dt_bias.reshape(1, -1), a_log, skip_gain.reshape(1, -1), ssm, w_mout, freq,
    )
    pad = -(-w_xproj.shape[1] // 128) * 128
    dma = pltpu.SemaphoreType.DMA
    buffers = [
        ((nz, rows, w_query.shape[1] + 128), BF16),
        ((2, rows, w_query.shape[1] + 128), F32),
        ((rows, w_query.shape[1] + 128), F32),
        ((rows, w_query.shape[1] + 128), F32),
        ((nz, rows, 2 * hd), F32),
        ((rows, hd), F32),
        ((rows, hd), F32),
        ((nz, qrows + 2, hd), BF16),
        ((nx, rows, feats), BF16),
        ((nz, rows, feats), BF16),
        ((nx, rows, pad), BF16),
        ((nz, rows, pad), BF16),
        ((nz, rows, feats), BF16),
        ((nz, rows, feats), BF16),
        ((nx, rows, feats), F32),
    ]
    flag = pltpu.SemaphoreType.REGULAR
    sems = [dma((nz,)), dma((nz,)), dma((2,)), dma((2,)), flag((3,)), flag, flag] + [dma] * 6 + [dma, dma((3,))] + [dma] * 8
    hidden, state = pl.pallas_call(
        functools.partial(kernel, nz, nx),
        out_shape=(
            pltpu.VMEM((rows, feats), BF16),
            pltpu.VMEM(ssm.shape, F32),
        ),
        in_specs=[pl.BlockSpec(memory_space=pltpu.HBM)] * len(operands),
        out_specs=(pl.BlockSpec(memory_space=pltpu.VMEM), pl.BlockSpec(memory_space=pltpu.VMEM)),
        scratch_shapes=[pltpu.VMEM(o.shape, o.dtype) for o in operands]
        + [dma((len(operands) + 3,))]
        + [pltpu.VMEM(shape, kind) for shape, kind in buffers]
        + sems,
        compiler_params=pltpu.CompilerParams(
            collective_id=0, has_side_effects=True, vmem_limit_bytes=48 * 2**20
        ),
        name="decode_step",
    )(*[pltpu.with_memory_space_constraint(o, pltpu.HBM) for o in operands])
    return pl.pallas_call(
        put_out,
        out_shape=(jax.ShapeDtypeStruct((rows, feats), BF16), jax.ShapeDtypeStruct(ssm.shape, F32)),
        in_specs=[pl.BlockSpec(memory_space=pltpu.VMEM)] * 2,
        out_specs=(pl.BlockSpec(memory_space=pltpu.HBM), pl.BlockSpec(memory_space=pltpu.HBM)),
        scratch_shapes=[dma((2,))],
        name="put_out",
        compiler_params=pltpu.CompilerParams(vmem_limit_bytes=2**20),
    )(*[pltpu.with_memory_space_constraint(o, pltpu.VMEM) for o in (hidden, state)])


def solution(mesh):
    batch = ("rep", "sub")
    chan = ("seq", "head")
    in_specs = (
        P(batch, "seq"), P("seq"), P("seq", "head"), P("seq", "head"), P("seq", "head"), P("head", "seq"),
        P(batch, "head", "seq", None), P(batch, "head", "seq", None), P(batch), P(batch), P(), P(None, None, chan),
        P(None, chan), P(chan), P(batch, None, chan), P(chan, None), P(None, chan), P(chan), P(None, chan), P(chan),
        P(batch, None, chan), P(chan, None),
    )
    out_specs = (P(batch, "seq"), P(batch, None, chan))
    body = functools.partial(local, mesh.shape["seq"], mesh.shape["head"])
    return jax.shard_map(body, mesh=mesh, in_specs=in_specs, out_specs=out_specs, check_vma=False)
```

```python
import functools
import math

import jax
import jax.numpy as jnp
import numpy as np
from jax import lax
from jax.experimental import pallas as pl
from jax.experimental.pallas import tpu as pltpu
from jax.sharding import PartitionSpec as P

NORM_EPS = 1e-05
FLOOR = -1e30
ROPE_BASE = 10000.0
MESH = pl.DeviceIdType.MESH
F32 = jnp.float32
BF16 = jnp.bfloat16


def far_first(n):
    return sorted(range(1, n), key=lambda k: -min(k, n - k))


def near_first(n):
    return far_first(n)[::-1]


def dot(a, b):
    return lax.dot_general(a, b, (((1,), (0,)), ((), ())), preferred_element_type=F32)


def dot_t(a, b):
    return lax.dot_general(a, b, (((1,), (1,)), ((), ())), preferred_element_type=F32)


def diagonal(shape):
    return lax.broadcasted_iota(jnp.int32, shape, 0) == lax.broadcasted_iota(jnp.int32, shape, 1)


def column_to_row(column):
    rows = column.shape[0]
    spread = jnp.where(diagonal((rows, 128)), jnp.broadcast_to(column, (rows, 128)), 0.0)
    return jnp.sum(spread, axis=0, keepdims=True)


def row_to_column(row, rows):
    spread = jnp.where(diagonal((rows, row.shape[1])), jnp.broadcast_to(row, (rows, row.shape[1])), 0.0)
    return jnp.sum(spread, axis=1, keepdims=True)


def in_terms(row, count):
    lane = lax.broadcasted_iota(jnp.int32, row.shape, 1)
    left = jnp.where(lane < count, row, 0.0)
    terms = jnp.zeros_like(row)
    for i in range(3):
        term = left.astype(BF16).astype(F32)
        terms = terms + (pltpu.roll(term, i * count, 1) if i else term)
        left = left - term
    return terms


def of_terms(terms, count):
    return terms + pltpu.roll(terms, 128 - count, 1) + pltpu.roll(terms, 128 - 2 * count, 1)


def send_all(axis, n, buffer, send_sem, recv_sem):
    me = lax.axis_index(axis)
    for k in far_first(n):
        pltpu.make_async_remote_copy(
            src_ref=buffer.at[0],
            dst_ref=buffer.at[k],
            send_sem=send_sem,
            recv_sem=recv_sem(k) if callable(recv_sem) else recv_sem,
            device_id={axis: lax.rem(me + k, n)},
            device_id_type=MESH,
        ).start()


def wait_for(buffer, sem, slots):
    part = buffer.at[pl.ds(0, slots)]
    pltpu.make_async_copy(part, part, sem).wait()


def kernel(nz, nx, *refs):
    (
        tokens_h, attn_gain_h, w_query_h, w_key_h, w_value_h, w_out_h, keys_h, values_h, lengths_h, positions_h,
        mamba_gain_h, w_in_h, conv_weight_h, conv_bias_h, conv_state_h, w_xproj_h, w_dt_h, dt_bias_h, a_log_h,
        skip_gain_h, ssm_h, w_mout_h, freq_h,
        hidden_o, state_o,
        tokens, attn_gain, w_query, w_key, w_value, w_out, keys, values, lengths, positions,
        mamba_gain, w_in, conv_weight, conv_bias, conv_state, w_xproj, w_dt, dt_bias, a_log,
        skip_gain, ssm, w_mout, freq,
        load_sem,
        turned, q_buf, below, up_to, total_q, kv_buf, knew, vnew, acc_buf, part_buf, mid_buf, px_buf, pz_buf,
        out_src, share_buf, fin_buf,
        s_q, r_q, s_up, r_up, go, ready_x, ready, s_kv, r_kv, s_acc, r_acc, s_part, r_part, s_mid, r_mid,
        s_px, r_px, s_pz, r_pz, s_sh, r_sh, s_fin, r_fin,
    ) = refs
    z = lax.axis_index("seq")
    x = lax.axis_index("head")
    first = jnp.where(x == 0, 1, 0)
    place = lax.rem(z + nz - first, nz)
    up = lax.rem(z + 1, nz)
    is_owner = place == 0

    loads = {}
    pairs = dict(
        tokens=(tokens_h, tokens), attn_gain=(attn_gain_h, attn_gain), w_query=(w_query_h, w_query), w_key=(w_key_h, w_key),
        w_value=(w_value_h, w_value), positions=(positions_h, positions), freq=(freq_h, freq), lengths=(lengths_h, lengths),
        keys=(keys_h, keys), values=(values_h, values), w_out=(w_out_h, w_out), mamba_gain=(mamba_gain_h, mamba_gain),
        w_in=(w_in_h, w_in), conv_weight=(conv_weight_h, conv_weight), conv_bias=(conv_bias_h, conv_bias),
        conv_state=(conv_state_h, conv_state), w_xproj=(w_xproj_h, w_xproj), w_dt=(w_dt_h, w_dt), dt_bias=(dt_bias_h, dt_bias),
        a_log=(a_log_h, a_log), skip_gain=(skip_gain_h, skip_gain), ssm=(ssm_h, ssm), w_mout=(w_mout_h, w_mout),
    )
    quarter = w_query.shape[0] // 4
    del pairs["w_query"]
    for i in range(4):
        part = pl.ds(i * quarter, quarter)
        loads["w_query", i] = pltpu.make_async_copy(w_query_h.at[part], w_query.at[part], load_sem.at[len(pairs) + i])
        loads["w_query", i].start()
    for i, (name, (source, target)) in enumerate(pairs.items()):
        loads[name] = pltpu.make_async_copy(source, target, load_sem.at[i])
        loads[name].start()

    def need(*names):
        for name in names:
            loads.pop(name).wait()

    barrier = pltpu.get_barrier_semaphore()

    def hub(k):
        peer = lax.rem(x + k, nx)
        return {"head": peer, "seq": jnp.where(peer == 0, 1, 0)}


    @pl.when(place == 0)
    def _():
        for k in far_first(nx):
            pl.semaphore_signal(barrier, inc=1, device_id=hub(k), device_id_type=MESH)

    pl.semaphore_wait(barrier, jnp.where(place == 0, nx - 1, 1))

    @pl.when(place < nz - 1)
    def _():
        pl.semaphore_signal(barrier, inc=1, device_id={"seq": up}, device_id_type=MESH)

    for i in (1, 2):

        @pl.when(place >= i)
        def _(i=i):
            pl.semaphore_signal(go.at[i], inc=1, device_id={"seq": lax.rem(z + nz - i, nz)}, device_id_type=MESH)

    rows = tokens.shape[0]
    feats = tokens.shape[1]
    hd = keys.shape[2]
    span = keys.shape[1]
    groups = w_query.shape[1] // hd
    qrows = groups * rows
    width = feats * nz
    chans = w_xproj.shape[0]
    rank = w_dt.shape[1]
    nstate = a_log.shape[0]

    need("tokens", "attn_gain", *[("w_query", i) for i in range(4)])
    token_f = tokens[...].astype(F32)
    lifted = (token_f * attn_gain[...]).astype(BF16)
    qw = w_query.shape[1]
    part = dot(lifted, w_query[...])
    q_buf[0, :, :qw] = part.astype(BF16)
    left = jnp.sum(token_f * token_f, axis=1, keepdims=True)
    lane = lax.broadcasted_iota(jnp.int32, (rows, 128), 1)
    up_to[:, :qw] = part
    up_to[:, qw:] = jnp.where(lane == 0, left, 0.0)
    terms = jnp.zeros((rows, 128), F32)
    for i in range(3):
        term = left.astype(BF16).astype(F32)
        terms = jnp.where(lane == i, term, terms)
        left = left - term
    q_buf[0, :, qw:] = terms.astype(BF16)

    for k in far_first(nz):

        @pl.when(place >= k)
        def _(k=k):
            pltpu.make_async_remote_copy(
                src_ref=q_buf.at[0], dst_ref=q_buf.at[k], send_sem=s_q.at[k], recv_sem=r_q.at[k],
                device_id={"seq": lax.rem(z + nz - k, nz)}, device_id_type=MESH,
            ).start()

    need("w_key", "w_value")
    kv_buf[0, :, :hd] = dot(lifted, w_key[...])
    kv_buf[0, :, hd:] = dot(lifted, w_value[...])

    @pl.when(place > 0)
    def _():
        pltpu.make_async_remote_copy(
            src_ref=kv_buf.at[0], dst_ref=kv_buf.at[place], send_sem=s_kv, recv_sem=r_kv,
            device_id={"seq": first}, device_id_type=MESH,
        ).start()

    knew[...] = jnp.zeros_like(knew)
    vnew[...] = jnp.zeros_like(vnew)
    need("positions", "freq", "lengths")
    angle = row_to_column(positions[...].astype(F32), rows) * freq[...]
    cosine = jnp.cos(angle)
    sine = jnp.sin(angle)
    cosine = jnp.concatenate([cosine, cosine], axis=1)
    sine = jnp.concatenate([-sine, sine], axis=1)

    def rotated(v):
        return v * cosine + pltpu.roll(v, hd // 2, 1) * sine

    limit = row_to_column(lengths[...].astype(F32), rows)
    limit = jnp.concatenate([limit] * groups, axis=0)
    spot = (lax.broadcasted_iota(jnp.int32, (qrows, span), 1) + z * span).astype(F32)
    live = spot < limit
    row_of = lax.broadcasted_iota(jnp.int32, (qrows, hd), 0) % rows
    row_of_wide = lax.broadcasted_iota(jnp.int32, (qrows, span), 0) % rows

    @pl.when(place >= 2)
    def _():
        pltpu.make_async_copy(below.at[1], below.at[1], r_up.at[1]).wait()
        up_to[...] += below[1]

    total_q[...] = up_to[...]

    for i in (1, 2):

        @pl.when(place < nz - i)
        def _(i=i):
            pl.semaphore_wait(go.at[i], 1)
            pltpu.make_async_remote_copy(
                src_ref=up_to, dst_ref=below.at[i - 1], send_sem=s_up.at[i - 1], recv_sem=r_up.at[i - 1],
                device_id={"seq": lax.rem(z + i, nz)}, device_id_type=MESH,
            ).start()

    need("keys")
    for b in range(rows):
        turned[b * hd : (b + 1) * hd] = keys[b].T

    @pl.when(place >= 1)
    def _():
        pltpu.make_async_copy(below.at[0], below.at[0], r_up.at[0]).wait()
        total_q[...] += below[0]

    for k in range(1, nz):

        @pl.when(place + k < nz)
        def _(k=k):
            pltpu.make_async_copy(q_buf.at[k], q_buf.at[k], r_q.at[k]).wait()
            total_q[...] += q_buf[k].astype(F32)

    @pl.when(place == 0)
    def _():
        for k in far_first(nx):
            pl.semaphore_signal(ready_x, inc=1, device_id=hub(k), device_id_type=MESH)

    r_a = lax.rsqrt(jnp.sum(total_q[:, qw:], axis=1, keepdims=True) / width + NORM_EPS)

    @pl.when(is_owner)
    def _():
        wait_for(kv_buf, r_kv, nz - 1)
        kv = kv_buf[0]
        for k in range(1, nz):
            kv = kv + kv_buf[k]
        knew[...] = rotated(kv[:, :hd] * r_a).astype(BF16).astype(F32)
        vnew[...] = (kv[:, hd:] * r_a).astype(BF16).astype(F32)

    q = [rotated(total_q[:, g * hd : (g + 1) * hd] * r_a) for g in range(groups)]
    q = jnp.concatenate(q, axis=0).astype(BF16)

    q = q.astype(F32)
    scale = hd ** (-0.5)
    scores = dot(jnp.concatenate([jnp.where(row_of == b, q, 0.0).astype(BF16) for b in range(rows)], axis=1), turned[...])
    scores = scores * scale
    top = jnp.max(jnp.where(live, scores, FLOOR), axis=1, keepdims=True)
    fresh = jnp.sum(q * jnp.concatenate([knew[...]] * groups, axis=0), axis=1, keepdims=True) * scale
    mine = jnp.broadcast_to(is_owner, fresh.shape)
    top = jnp.maximum(top, jnp.where(mine, fresh, FLOOR))
    weights = jnp.where(live, jnp.exp(scores - top), 0.0)
    new_weight = jnp.where(mine, jnp.exp(fresh - top), 0.0)
    total = jnp.sum(weights, axis=1, keepdims=True) + new_weight
    weights = jnp.concatenate([jnp.where(row_of_wide == b, weights, 0.0).astype(BF16) for b in range(rows)], axis=1)
    need("values")
    acc = dot(weights, values[...].reshape(rows * span, hd))
    acc = acc + new_weight * jnp.concatenate([vnew[...]] * groups, axis=0)
    acc_buf[0, :qrows] = acc.astype(BF16)
    acc_buf[0, qrows:] = jnp.concatenate([in_terms(column_to_row(top), qrows), in_terms(column_to_row(total), qrows)]).astype(BF16)
    send_all("seq", nz, acc_buf, s_acc, r_acc)

    @pl.when(place == 0)
    def _():
        pl.semaphore_wait(ready_x, nx - 1)
        for k in far_first(nz):
            pl.semaphore_signal(ready, inc=1, device_id={"seq": lax.rem(z + k, nz)}, device_id_type=MESH)


    need("w_out")
    wait_for(acc_buf, r_acc, nz - 1)
    aux = [acc_buf[k, qrows:].astype(F32) for k in range(nz)]
    tops = of_terms(jnp.concatenate([a[:1] for a in aux], axis=0), qrows)
    sums = of_terms(jnp.concatenate([a[1:] for a in aux], axis=0), qrows)
    factor = jnp.exp(tops - jnp.max(tops, axis=0, keepdims=True))
    whole = jnp.sum(factor * sums, axis=0, keepdims=True)
    lane = lax.broadcasted_iota(jnp.int32, (nz, 128), 1)
    share = jnp.where(lane < qrows, factor / whole, 0.0)
    share = share.T
    attended = share[:qrows, 0:1] * acc_buf[0, :qrows].astype(F32)
    for k in range(1, nz):
        attended = attended + share[:qrows, k : k + 1] * acc_buf[k, :qrows].astype(F32)
    attended = jnp.concatenate([attended[g * rows : (g + 1) * rows] for g in range(groups)], axis=1).astype(BF16)
    part_buf[0] = dot(attended, w_out[...]).astype(BF16)

    @pl.when(place > 0)
    def _():
        pl.semaphore_wait(ready, 1)

    send_all("head", nx, part_buf, s_part, r_part)
    need("mamba_gain", "w_in")
    wait_for(part_buf, r_part, nx - 1)
    summed = part_buf[lax.rem(x, nx)].astype(F32)
    for j in range(1, nx):
        summed = summed + part_buf[lax.rem(x - j + nx, nx)].astype(F32)
    mid = (token_f + summed).astype(BF16)
    mid_buf[0] = mid
    circle = sorted(range(1, nz), key=lambda k: min(k, nz - k))
    ends = (0, nz // 2, max(nz // 2, nz - 4), nz - 1)
    rings = [circle[i:j] for i, j in zip(ends, ends[1:]) if j > i]
    ring_of = {k: i for i, r in enumerate(rings) for k in r}
    send_all("seq", nz, mid_buf, s_mid, lambda k: r_mid.at[ring_of[k]])

    def block_of(k):
        at = pl.multiple_of(lax.rem(z - k + nz, nz) * feats, feats)
        block = mid_buf[k].astype(F32)
        raised = (block * mamba_gain[:, pl.ds(at, feats)]).astype(BF16)
        return block * block, dot_t(raised, w_in[:, pl.ds(at, feats)])

    squares, both = block_of(0)
    for i, ring in enumerate(rings):
        wait_for(mid_buf, r_mid.at[i], len(ring))
        for k in ring:
            more, extra = block_of(k)
            squares = squares + more
            both = both + extra
    both = both * lax.rsqrt(jnp.sum(squares, axis=1, keepdims=True) / width + NORM_EPS)
    inner = both[:, :chans]
    gate = both[:, chans:]

    need("conv_weight", "conv_bias", "conv_state", "w_xproj")
    mixed = inner * conv_weight[3:4, :] + conv_bias[...]
    for k in range(3):
        mixed = mixed + conv_state[k] * conv_weight[k : k + 1, :]
    u = mixed / (1.0 + jnp.exp(-mixed))
    proj = dot(u.astype(BF16), w_xproj[...])
    px_buf[0] = jnp.concatenate([proj, jnp.zeros((rows, px_buf.shape[2] - proj.shape[1]), F32)], axis=1).astype(BF16)
    send_all("head", nx, px_buf, s_px, r_px)
    need("w_dt", "dt_bias", "a_log", "skip_gain", "ssm", "w_mout")
    decay_rate = -jnp.exp(a_log[...])
    gated = gate / (1.0 + jnp.exp(-gate))
    wait_for(px_buf, r_px, nx - 1)
    proj = px_buf[0].astype(F32)
    for k in range(1, nx):
        proj = proj + px_buf[k].astype(F32)
    pz_buf[0] = proj.astype(BF16)
    send_all("seq", nz, pz_buf, s_pz, r_pz)
    wait_for(pz_buf, r_pz, nz - 1)
    proj = pz_buf[0].astype(F32)
    for k in range(1, nz):
        proj = proj + pz_buf[k].astype(F32)

    pre = dot_t(proj[:, :rank].astype(BF16), w_dt[...]) + dt_bias[...]
    step = jnp.maximum(pre, 0.0) + jnp.log(1.0 + jnp.exp(-jnp.abs(pre)))
    maps = proj[:, rank : rank + 128].T
    drive = step * u
    reads = []
    for b in range(rows):
        state = (
            jnp.exp(step[b : b + 1, :] * decay_rate) * ssm[b]
            + drive[b : b + 1, :] * maps[:nstate, b : b + 1]
        )
        state_o[b] = state
        reads.append(jnp.sum(maps[nstate : 2 * nstate, b : b + 1] * state, axis=0, keepdims=True))
    y = (jnp.concatenate(reads, axis=0) + skip_gain[...] * u) * gated
    y = y.astype(BF16)

    def out_block(k):
        at = pl.multiple_of(lax.rem(z + k, nz) * feats, feats)
        return dot(y, w_mout[:, pl.ds(at, feats)]).astype(BF16)

    for k in far_first(nz):
        out_src[k] = out_block(k)
        pltpu.make_async_remote_copy(
            src_ref=out_src.at[k], dst_ref=share_buf.at[k], send_sem=s_sh, recv_sem=r_sh,
            device_id={"seq": lax.rem(z + k, nz)}, device_id_type=MESH,
        ).start()
    result = out_block(0).astype(F32)
    wait_for(share_buf, r_sh, nz - 1)
    for k in range(1, nz):
        result = result + share_buf[k].astype(F32)
    fin_buf[0] = result
    send_all("head", nx, fin_buf, s_fin, r_fin)

    for k in range(1, nz):

        @pl.when(place >= k)
        def _(k=k):
            pltpu.make_async_copy(q_buf.at[0], q_buf.at[0], s_q.at[k]).wait()

    @pl.when(place > 0)
    def _():
        pltpu.make_async_copy(kv_buf.at[0], kv_buf.at[0], s_kv).wait()

    for i in (1, 2):

        @pl.when(place < nz - i)
        def _(i=i):
            pltpu.make_async_copy(up_to, up_to, s_up.at[i - 1]).wait()

    wait_for(acc_buf, s_acc, nz - 1)
    wait_for(part_buf, s_part, nx - 1)
    wait_for(mid_buf, s_mid, nz - 1)
    wait_for(px_buf, s_px, nx - 1)
    wait_for(pz_buf, s_pz, nz - 1)
    wait_for(share_buf, s_sh, nz - 1)
    wait_for(fin_buf, r_fin, nx - 1)
    result = fin_buf[lax.rem(x, nx)]
    for j in range(1, nx):
        result = result + fin_buf[lax.rem(x - j + nx, nx)]
    hidden_o[...] = (mid.astype(F32) + result).astype(BF16)
    wait_for(fin_buf, s_fin, nx - 1)


def put_out(hidden, state, hidden_o, state_o, sem):
    copies = [pltpu.make_async_copy(hidden, hidden_o, sem.at[0]), pltpu.make_async_copy(state, state_o, sem.at[1])]
    for copy in copies:
        copy.start()
    for copy in copies:
        copy.wait()


def local(nz, nx, *args):
    (
        tokens, attn_gain, w_query, w_key, w_value, w_out, keys, values, lengths, positions, mamba_gain, w_in,
        conv_weight, conv_bias, conv_state, w_xproj, w_dt, dt_bias, a_log, skip_gain, ssm, w_mout,
    ) = args
    rows, feats = tokens.shape
    hd = keys.shape[3]
    span = keys.shape[2]
    half = hd // 2
    qrows = w_query.shape[1] // hd * rows
    two, width, chans = w_in.shape
    freq = jnp.asarray(np.exp(-math.log(ROPE_BASE) * 2.0 * np.arange(half) / (2 * half)).reshape(1, half), F32)
    operands = (
        tokens, attn_gain.reshape(1, -1), w_query, w_key, w_value, w_out,
        keys.reshape(rows, span, hd), values.reshape(rows, span, hd), lengths.reshape(1, -1), positions.reshape(1, -1),
        mamba_gain.reshape(1, -1), jnp.transpose(w_in, (0, 2, 1)).reshape(two * chans, width),
        conv_weight, conv_bias.reshape(1, -1), jnp.transpose(conv_state, (1, 0, 2)), w_xproj,
        jnp.transpose(w_dt), dt_bias.reshape(1, -1), a_log, skip_gain.reshape(1, -1), ssm, w_mout, freq,
    )
    pad = -(-w_xproj.shape[1] // 128) * 128
    dma = pltpu.SemaphoreType.DMA
    buffers = [
        ((rows * hd, span), BF16),
        ((nz, rows, w_query.shape[1] + 128), BF16),
        ((2, rows, w_query.shape[1] + 128), F32),
        ((rows, w_query.shape[1] + 128), F32),
        ((rows, w_query.shape[1] + 128), F32),
        ((nz, rows, 2 * hd), F32),
        ((rows, hd), F32),
        ((rows, hd), F32),
        ((nz, qrows + 2, hd), BF16),
        ((nx, rows, feats), BF16),
        ((nz, rows, feats), BF16),
        ((nx, rows, pad), BF16),
        ((nz, rows, pad), BF16),
        ((nz, rows, feats), BF16),
        ((nz, rows, feats), BF16),
        ((nx, rows, feats), F32),
    ]
    flag = pltpu.SemaphoreType.REGULAR
    sems = [dma((nz,)), dma((nz,)), dma((2,)), dma((2,)), flag((3,)), flag, flag] + [dma] * 6 + [dma, dma((3,))] + [dma] * 8
    hidden, state = pl.pallas_call(
        functools.partial(kernel, nz, nx),
        out_shape=(
            pltpu.VMEM((rows, feats), BF16),
            pltpu.VMEM(ssm.shape, F32),
        ),
        in_specs=[pl.BlockSpec(memory_space=pltpu.HBM)] * len(operands),
        out_specs=(pl.BlockSpec(memory_space=pltpu.VMEM), pl.BlockSpec(memory_space=pltpu.VMEM)),
        scratch_shapes=[pltpu.VMEM(o.shape, o.dtype) for o in operands]
        + [dma((len(operands) + 3,))]
        + [pltpu.VMEM(shape, kind) for shape, kind in buffers]
        + sems,
        compiler_params=pltpu.CompilerParams(
            collective_id=0, has_side_effects=True, vmem_limit_bytes=48 * 2**20
        ),
        name="decode_step",
    )(*[pltpu.with_memory_space_constraint(o, pltpu.HBM) for o in operands])
    return pl.pallas_call(
        put_out,
        out_shape=(jax.ShapeDtypeStruct((rows, feats), BF16), jax.ShapeDtypeStruct(ssm.shape, F32)),
        in_specs=[pl.BlockSpec(memory_space=pltpu.VMEM)] * 2,
        out_specs=(pl.BlockSpec(memory_space=pltpu.HBM), pl.BlockSpec(memory_space=pltpu.HBM)),
        scratch_shapes=[dma((2,))],
        name="put_out",
        compiler_params=pltpu.CompilerParams(vmem_limit_bytes=2**20),
    )(*[pltpu.with_memory_space_constraint(o, pltpu.VMEM) for o in (hidden, state)])


def solution(mesh):
    batch = ("rep", "sub")
    chan = ("seq", "head")
    in_specs = (
        P(batch, "seq"), P("seq"), P("seq", "head"), P("seq", "head"), P("seq", "head"), P("head", "seq"),
        P(batch, "head", "seq", None), P(batch, "head", "seq", None), P(batch), P(batch), P(), P(None, None, chan),
        P(None, chan), P(chan), P(batch, None, chan), P(chan, None), P(None, chan), P(chan), P(None, chan), P(chan),
        P(batch, None, chan), P(chan, None),
    )
    out_specs = (P(batch, "seq"), P(batch, None, chan))
    body = functools.partial(local, mesh.shape["seq"], mesh.shape["head"])
    return jax.shard_map(body, mesh=mesh, in_specs=in_specs, out_specs=out_specs, check_vma=False)
```
